256 devices in a mesh: seq: 32 (over y, x, core), head: 8 (over z).
Axes of the slice: x: 4, y: 4, z: 8, core: 2. Of those that a mesh axis runs over, the one named last changes fastest.
Arguments:
- patch_embed: bfloat16 [32, 1024, 1280], P('head', 'seq'), may hold values from -6 to 6
- perturbation: float32 [32, 1024, 1280], P('head', 'seq'), may hold values from -3 to 3
- target: bfloat16 [32, 1024, 1280], P('head', 'seq'), may hold values from -6 to 6
- ln_gain: float32 [1280], replicated, may hold values from 0.5 to 1.5
- ln_bias: float32 [1280], replicated, may hold values from -1.5 to 1.5
- w_qkv: bfloat16 [16, 240, 1280], P('head'), may hold values from -10.0623059 to 10.0623059
- w_out: bfloat16 [16, 80, 1280], P('head'), may hold values from -0.15625 to 0.15625
- radius: float32 [32], replicated, may hold values from 137.38402 to 423.6007
- step_size: float32 [32], replicated, may hold values from 34.346004 to 137.38402
Outputs:
- perturbation_out: float32 [32, 1024, 1280], P('head', 'seq')
The draws below stay inside these ranges and needn't reach their ends.
All inputs are finite; a program needn't handle non-finite values.
Results may differ from the reference program's by a relative error of at most 0.001.
Values may be sent and summed in bfloat16 or wider, within the bound.
A program may use at most 64 MiB of HBM per device.

```python
import math
import jax
import jax.numpy as jnp
from jax import lax

D = 1280
HEADS = 16
HD = 80
PATCHES = 1024
PGD_STEPS = 1
EXAMPLES = 32


def draw_w_qkv(key, part):
    entries = jax.random.truncated_normal(key, -6.0, 6.0, (HEADS, 3 * HD, D), jnp.float32) / math.sqrt(D)
    return entries.astype(jnp.bfloat16)


def levels(stream_key, dims, shards, smallest, top_value):
    def one(position, parts):
        steps = jax.random.uniform(jax.random.fold_in(jax.random.fold_in(stream_key, 6), position), (parts,), jnp.float32, smallest / len(shards), top_value / len(shards))
        return jnp.repeat(jnp.exp(steps), dims[position] // parts).reshape((-1,) + (1,) * (len(dims) - position - 1))

    gain = one(*shards[0])
    for cut in shards[1:]:
        gain = gain * one(*cut)
    return gain


def gaussian(own_key, extent, scale, limit, shards=(), held_as=jnp.bfloat16):
    values = scale * jax.random.normal(own_key, extent, jnp.float32)
    if shards:
        values = values * levels(own_key, extent, shards, -0.22, 0.18)
    return jnp.clip(values, -limit, limit).astype(held_as)


def setup_inputs(seed: int = 0) -> dict:
    splits = jax.random.split(jax.random.key(seed), 10)
    return {
        "patch_embed": gaussian(splits[0], (EXAMPLES, PATCHES, D), 1.0, 6.0, ((0, 8), (1, 32))),
        "perturbation": gaussian(splits[1], (EXAMPLES, PATCHES, D), 0.5, 3.0, ((0, 8), (1, 32)), jnp.float32),
        "target": gaussian(splits[2], (EXAMPLES, PATCHES, D), 1.0, 6.0, ((0, 8), (1, 32))),
        "ln_gain": jnp.clip(1.0 + 0.1 * jax.random.normal(splits[3], (D,), jnp.float32), 0.5, 1.5),
        "ln_bias": gaussian(splits[4], (D,), 0.3, 1.5, (), jnp.float32),
        "w_qkv": draw_w_qkv(jax.random.fold_in(splits[9], 71), 0),
        "w_out": gaussian(splits[6], (HEADS, HD, D), (HEADS * HD) ** -0.5, 0.15625, ((0, 8),)),
        "radius": jnp.clip(jnp.exp(jax.random.uniform(splits[7], (EXAMPLES,), jnp.float32, math.log(137.38402), math.log(423.6007))), 137.38402, 423.6007),
        "step_size": jnp.clip(jnp.exp(jax.random.uniform(splits[8], (EXAMPLES,), jnp.float32, math.log(34.346004), math.log(137.38402))), 34.346004, 137.38402),
    }


norm_epsilon = 1e-06
layer_epsilon = 1e-06

def layer_statistics(gathered):
    center = gathered - lax.optimization_barrier(jnp.mean(gathered, axis=-1, keepdims=True))
    variance = lax.optimization_barrier(jnp.mean(center * center, axis=-1, keepdims=True))
    inverse = lax.rsqrt(variance + layer_epsilon)
    return (center * inverse, inverse)

def forward_pair(packed):
    score_scale = 1.0 / math.sqrt(HD)
    queries = packed[:, :HD]
    key_rows = packed[:, HD:2 * HD]
    values = packed[:, 2 * HD:]
    scores = jnp.dot(queries, key_rows.T, preferred_element_type=jnp.float32) * score_scale
    row_max = lax.optimization_barrier(jnp.max(scores, axis=-1, keepdims=True))
    log_total = row_max + jnp.log(lax.optimization_barrier(jnp.sum(jnp.exp(scores - row_max), axis=-1, keepdims=True)))
    weights = jnp.exp(scores - log_total).astype(jnp.bfloat16)
    output = jnp.dot(weights, values, preferred_element_type=jnp.float32).astype(jnp.bfloat16)
    return (output, log_total[:, 0])

def backward_pair(inputs):
    packed, output, log_total, grad_output = inputs
    score_scale = 1.0 / math.sqrt(HD)
    queries = packed[:, :HD]
    key_rows = packed[:, HD:2 * HD]
    values = packed[:, 2 * HD:]
    scores = jnp.dot(queries, key_rows.T, preferred_element_type=jnp.float32) * score_scale
    weights = jnp.exp(scores - log_total[:, None])
    row_dot = lax.optimization_barrier(jnp.sum(grad_output.astype(jnp.float32) * output.astype(jnp.float32), axis=-1))
    grad_values = jnp.dot(weights.astype(jnp.bfloat16).T, grad_output, preferred_element_type=jnp.float32)
    grad_weights = jnp.dot(grad_output, values.T, preferred_element_type=jnp.float32)
    grad_scores = (weights * (grad_weights - row_dot[:, None]) * score_scale).astype(jnp.bfloat16)
    grad_query = jnp.dot(grad_scores, key_rows, preferred_element_type=jnp.float32)
    grad_keys = jnp.dot(grad_scores.T, queries, preferred_element_type=jnp.float32)
    return jnp.concatenate([grad_query.astype(jnp.bfloat16), grad_keys.astype(jnp.bfloat16), grad_values.astype(jnp.bfloat16)], axis=-1)

def reference(patch_embed, perturbation, target, ln_gain, ln_bias, w_qkv, w_out, radius, step_size):
    highest = lax.Precision.HIGHEST
    weights_in = w_qkv.astype(jnp.float32)
    weights_back = w_out.astype(jnp.float32)
    current = perturbation
    for attempt in range(PGD_STEPS):
        mixed = patch_embed.astype(jnp.float32) + current
        rounded = lax.optimization_barrier(mixed.astype(jnp.bfloat16))
        normed, inverse = layer_statistics(rounded.astype(jnp.float32))
        hidden = (normed * ln_gain + ln_bias).astype(jnp.bfloat16)
        packed = jnp.einsum('epd,hcd->ehpc', hidden.astype(jnp.float32), weights_in, precision=highest).astype(jnp.bfloat16)
        pair_rows = packed.reshape(EXAMPLES * HEADS, PATCHES, 3 * HD)
        output, log_total = lax.map(forward_pair, pair_rows)
        output_heads = output.reshape(EXAMPLES, HEADS, PATCHES, HD)
        branch = jnp.einsum('ehpc,hcd->epd', output_heads.astype(jnp.float32), weights_back, precision=highest)
        result = mixed + branch
        residual = result - target.astype(jnp.float32)
        residual_half = residual.astype(jnp.bfloat16)
        grad_output = jnp.einsum('epd,hcd->ehpc', residual_half.astype(jnp.float32), weights_back, precision=highest).astype(jnp.bfloat16)
        grad_packed = lax.map(backward_pair, (pair_rows, output, log_total, grad_output.reshape(EXAMPLES * HEADS, PATCHES, HD)))
        grad_packed = grad_packed.reshape(EXAMPLES, HEADS, PATCHES, 3 * HD)
        grad_hidden = jnp.einsum('ehpc,hcd->epd', grad_packed.astype(jnp.float32), weights_in, precision=highest)
        scaled = grad_hidden * ln_gain
        first_mean = lax.optimization_barrier(jnp.mean(scaled, axis=-1, keepdims=True))
        second_mean = lax.optimization_barrier(jnp.mean(scaled * normed, axis=-1, keepdims=True))
        grad_input = (scaled - first_mean - normed * second_mean) * inverse
        gradient = residual + grad_input
        grad_square = lax.optimization_barrier(jnp.sum(gradient * gradient, axis=(1, 2)))
        stepped = current + (step_size / jnp.sqrt(grad_square + norm_epsilon))[:, None, None] * gradient
        stepped_square = lax.optimization_barrier(jnp.sum(stepped * stepped, axis=(1, 2)))
        current = stepped * jnp.minimum(1.0, radius / jnp.sqrt(stepped_square + norm_epsilon))[:, None, None]
    return current
```

```python
import functools
import math

import jax
import jax.numpy as jnp
from jax import lax
from jax.experimental import pallas as pl
from jax.experimental.pallas import tpu as pltpu
from jax.sharding import PartitionSpec as P

norm_epsilon = 1e-06
layer_epsilon = 1e-06

F32 = jnp.float32
BF16 = jnp.bfloat16
NT = (((1,), (1,)), ((), ()))
NN = (((1,), (0,)), ((), ()))
TN = (((0,), (0,)), ((), ()))

IMAGES = 4
ROWS = 4
COLS = 4
PLANES = 8
SEQ = 32
BLOCK = 32
WIDTH = 1280
HD = 80
PAD = 128
CHUNK = 40
NB = 256
NSTEPS = WIDTH // NB
TILE = 256


def dot(a, b, dims):
    return lax.dot_general(a, b, dims, preferred_element_type=F32)


def shard_offset(x, c):
    other = 8 - x - 4 * (1 - (x + 3) // 4)
    return (1 - c) * x + c * other


def kernel(
    pe, pert, tgt, gain, bias, w_own, wo_own, rad, stp, out,
    H, Wp, W2, WO, normed, inv, HS, Q, K, V, O, OR, LSE, GS, GO, GQ, GP, GP2,
    RES, PF, PB, R1L, R1R, S2L, S2R, R2L, R2R, YS, YR, SC, SCR,
    s_wz, r_wz, s_wy, r_wyl, r_wyr, r_wyy, s_hy, r_hy, s_hx, r_hxl, r_hxr, r_hxy, r_hxz,
    s_hd, r_hd, s_wo, r_wo, s_wod, r_wod, l_wo, s_wd, r_wd, s_oa, r_oa, s_ga, r_ga,
    s_gp, r_gp, s_r1, r_r1l, r_r1r, s_r2, r_r2l, r_r2r, s_ry, r_ry, s_sc, r_sc,
):
    s = lax.axis_index("seq")
    z = lax.axis_index("head")
    y = s // 8
    x = (s // 2) % 4
    c = s % 2
    k8 = s % 8

    def at(yy, xx, cc):
        return (yy * 4 + xx) * 2 + cc

    right = at(y, (x + 1) % 4, c)
    left = at(y, (x + 3) % 4, c)
    down = at((y + 1) % 4, x, c)
    up = at((y + 3) % 4, x, c)
    partner = at(y, x, 1 - c)

    def send(src, dst, ssem, rsem, **where):
        copy = pltpu.make_async_remote_copy(
            src_ref=src, dst_ref=dst, send_sem=ssem, recv_sem=rsem,
            device_id=where, device_id_type=pl.DeviceIdType.MESH,
        )
        copy.start()

    def arrived(ref, sem):
        pltpu.make_async_copy(ref, ref, sem).wait()

    barrier = pltpu.get_barrier_semaphore()

    @pl.loop(1, SEQ)
    def _(d):
        pl.semaphore_signal(
            barrier, inc=1, device_id={"seq": (s + d) % SEQ}, device_id_type=pl.DeviceIdType.MESH
        )

    @pl.loop(1, PLANES)
    def _(d):
        pl.semaphore_signal(
            barrier, inc=1, device_id={"head": (z + d) % PLANES},
            device_id_type=pl.DeviceIdType.MESH,
        )

    own_wo = pltpu.make_async_copy(wo_own, WO.at[z, :, pl.ds(0, HD)], l_wo)
    own_wo.start()

    @pl.loop(0, 6)
    def _(t):
        Wp[t, HD:PAD, :] = jnp.zeros((PAD - HD, WIDTH), BF16)

    @pl.loop(0, 16)
    def _(t):
        WO[t // 2, t % 2, HD:PAD, :] = jnp.zeros((PAD - HD, WIDTH), BF16)

    def layer_norm(image):
        mixed = pe[image].astype(F32) + pert[image]
        rounded = mixed.astype(BF16).astype(F32)
        center = rounded - jnp.mean(rounded, axis=-1, keepdims=True)
        variance = jnp.mean(center * center, axis=-1, keepdims=True)
        inverse = lax.rsqrt(variance + layer_epsilon)
        unit = center * inverse
        normed[image] = unit
        inv[image] = jnp.broadcast_to(inverse, (BLOCK, PAD))
        RES[image] = mixed - tgt[image].astype(F32)
        return (unit * gain[...] + bias[...]).astype(BF16)

    @pl.loop(1, ROWS)
    def _(d):
        image = (y + d) % 4
        HS[image] = layer_norm(image)

    H[y, x, c] = layer_norm(y)

    pl.semaphore_wait(barrier, SEQ - 1 + PLANES - 1)

    offset = shard_offset(x, c)
    target = (z + 8 - offset) % 8

    def chunk(yy, j):
        u = 3 * yy + j
        return Wp.at[u // 2, pl.ds(pl.multiple_of(CHUNK * (u % 2), 8), CHUNK)]

    for j in range(3):
        @pl.when(offset == 0)
        def _():
            pltpu.make_async_copy(w_own.at[3 * y + j], chunk(y, j), r_wz.at[j]).start()

        @pl.when(offset != 0)
        def _():
            send(w_own.at[3 * y + j], chunk(y, j), s_wz, r_wz.at[j], head=target)

    @pl.loop(1, ROWS)
    def _(d):
        image = (y + d) % 4
        send(HS.at[image], H.at[y, x, c], s_hy, r_hy.at[d - 1], seq=at(image, x, c))

    def spread(d):
        yy = (y + d) % 4
        block = H.at[yy, x, c]
        send(block, block, s_hx, r_hxl.at[d], seq=right)
        send(block, block, s_hx, r_hxr.at[d], seq=left)
        send(block, block, s_hd, r_hd.at[d * 4], seq=partner)

    spread(0)

    @pl.loop(1, ROWS)
    def _(d):
        arrived(H.at[(y + d) % 4, x, c], r_hy.at[3 - d])
        spread(d)

    for j in range(3):
        arrived(chunk(y, j), r_wz.at[j])
        send(chunk(y, j), chunk(y, j), s_wy, r_wyl.at[j], seq=down)
        send(chunk(y, j), chunk(y, j), s_wy, r_wyr.at[j], seq=up)

    @pl.loop(1, PLANES)
    def _(d):
        send(
            wo_own.at[c], WO.at[z, c, pl.ds(0, HD)], s_wo, r_wo.at[d],
            head=(z + d) % 8,
        )

    @pl.loop(0, ROWS)
    def _(d):
        yy = (y + d) % 4
        from_left = H.at[yy, (x + 3) % 4, c]
        arrived(from_left, r_hxl.at[d])
        upper = H.at[yy, (x + 3) % 4, c, pl.ds(0, 16)]
        send(upper, upper, s_hx, r_hxy.at[d], seq=right)
        send(from_left, from_left, s_hd, r_hd.at[d * 4 + 1], seq=partner)
        from_right = H.at[yy, (x + 1) % 4, c]
        arrived(from_right, r_hxr.at[d])
        lower = H.at[yy, (x + 1) % 4, c, pl.ds(16, 16)]
        send(lower, lower, s_hx, r_hxz.at[d], seq=left)
        send(from_right, from_right, s_hd, r_hd.at[d * 4 + 2], seq=partner)

    yu, yd, yo = (y + 3) % 4, (y + 1) % 4, (y + 2) % 4
    for j in range(3):
        arrived(chunk(yu, j), r_wyl.at[j])
        if j != 1:
            send(chunk(yu, j), chunk(yu, j), s_wy, r_wyy.at[j], seq=down)
        arrived(chunk(yd, j), r_wyr.at[j])
        if j == 1:
            send(chunk(yd, j), chunk(yd, j), s_wy, r_wyy.at[j], seq=up)

    @pl.loop(0, ROWS)
    def _(d):
        yy, xx = (y + d) % 4, (x + 2) % 4
        arrived(H.at[yy, xx, c, pl.ds(0, 16)], r_hxy.at[d])
        arrived(H.at[yy, xx, c, pl.ds(16, 16)], r_hxz.at[d])
        send(H.at[yy, xx, c], H.at[yy, xx, c], s_hd, r_hd.at[d * 4 + 3], seq=partner)

    for j in range(3):
        arrived(chunk(yo, j), r_wyy.at[j])

    send(Wp, W2, s_wd, r_wd, seq=partner)

    @pl.loop(0, ROWS)
    def _(d):
        yy = (y + d) % 4
        arrived(H.at[yy, x, 1 - c], r_hd.at[d * 4])
        arrived(H.at[yy, (x + 3) % 4, 1 - c], r_hd.at[d * 4 + 1])
        arrived(H.at[yy, (x + 1) % 4, 1 - c], r_hd.at[d * 4 + 2])
        arrived(H.at[yy, (x + 2) % 4, 1 - c], r_hd.at[d * 4 + 3])

    @pl.loop(0, 4)
    def _(t):
        rows = pl.ds(pl.multiple_of(t * 256, 256), 256)
        tokens = H[t].reshape(256, WIDTH)
        packed = dot(tokens, Wp[...].reshape(6 * PAD, WIDTH), NT).astype(BF16)
        for h in range(2):
            Q[h, rows] = packed[:, (3 * h) * PAD : (3 * h + 1) * PAD]
            K[h, rows] = packed[:, (3 * h + 1) * PAD : (3 * h + 2) * PAD]
            V[h, rows] = packed[:, (3 * h + 2) * PAD : (3 * h + 3) * PAD]

    scale = 1.0 / math.sqrt(HD)

    @pl.loop(0, 8)
    def _(t):
        h, row = t // 4, t % 4
        rows = pl.ds(pl.multiple_of(row * TILE, TILE), TILE)
        scores = dot(Q[h, rows], K[h], NT) * scale
        top = jnp.max(scores, axis=-1, keepdims=True)
        grown = jnp.exp(scores - top)
        total = jnp.sum(grown, axis=-1, keepdims=True)
        weights = (grown * (1.0 / total)).astype(BF16)
        part = dot(weights, V[h], NN).astype(BF16)
        O[h, row] = part.reshape(8, BLOCK, PAD)
        column = jnp.broadcast_to(top + jnp.log(total), (TILE, PAD))
        LSE[h, :, rows] = jnp.transpose(column)[0:8]

        @pl.loop(0, 8)
        def _(k):
            dest = row * 8 + k

            @pl.when(dest != s)
            def _():
                send(O.at[h, row, k], OR.at[h, y, k8], s_oa, r_oa, seq=dest)

    for h in range(2):
        OR[h, y, k8] = O[h, y, k8]

    @pl.loop(1, PLANES)
    def _(d):
        plane = (z + 8 - d) % 8
        piece = WO.at[plane, c, pl.ds(0, HD)]
        arrived(piece, r_wo.at[d])
        send(piece, piece, s_wod, r_wod.at[d], seq=partner)

    own_wo.wait()

    @pl.loop(1, PLANES)
    def _(d):
        plane = (z + 8 - d) % 8
        arrived(WO.at[plane, 1 - c, pl.ds(0, HD)], r_wod.at[d])

    flat_or = OR.reshape(64, BLOCK, PAD)
    arrived(flat_or.at[pl.ds(0, 62)], r_oa)

    @pl.loop(0, 8)
    def _(k):
        kk = (z + shard_offset((k // 2), k % 2)) % 8
        heads = jnp.concatenate([OR[h, :, k].reshape(128, PAD) for h in range(2)], axis=-1)
        branch = dot(heads, WO[kk].reshape(2 * PAD, WIDTH), NN)
        RES[...] += branch.reshape(IMAGES, BLOCK, WIDTH)

    @pl.loop(0, 8)
    def _(k):
        kk = (z + shard_offset((k // 2), k % 2)) % 8
        half = RES[...].reshape(128, WIDTH).astype(BF16)
        back = dot(half, WO[kk].reshape(2 * PAD, WIDTH), NT).astype(BF16)
        for h in range(2):
            GS[h, :, k] = back[:, h * PAD : (h + 1) * PAD].reshape(IMAGES, BLOCK, PAD)

        @pl.loop(0, IMAGES)
        def _(i):
            dest = i * 8 + k

            @pl.when(dest != s)
            def _():
                for h in range(2):
                    send(GS.at[h, i, k], GO.at[h, s], s_ga, r_ga, seq=dest)

    for h in range(2):
        GO[h, s] = GS[h, y, k8]

    flat_go = GO.reshape(64, BLOCK, PAD)
    arrived(flat_go.at[pl.ds(0, 62)], r_ga)

    @pl.loop(0, 8)
    def _(t):
        h, row = t // 4, t % 4
        rows = pl.ds(pl.multiple_of(row * TILE, TILE), TILE)
        queries = Q[h]
        grads = GO[h].reshape(1024, PAD)
        outputs = O[h].reshape(1024, PAD)
        products = grads.astype(F32) * outputs.astype(F32)
        row_dot = jnp.sum(jnp.transpose(products), axis=0, keepdims=True)
        scores = dot(K[h, rows], queries, NT) * scale
        weights = jnp.exp(scores - LSE[h, 0:1])
        grad_values = dot(weights.astype(BF16), grads, NN)
        grad_weights = dot(V[h, rows], grads, NT)
        grad_scores = (weights * (grad_weights - row_dot) * scale).astype(BF16)
        grad_keys = dot(grad_scores, queries, NN)
        grad_query = dot(grad_scores, K[h, rows], TN)

        @pl.when(row == 0)
        def _():
            GQ[...] = grad_query

        @pl.when(row != 0)
        def _():
            GQ[...] += grad_query

        def store(block_row, kind, value):
            lanes = pl.ds(pl.multiple_of((h * 3 + kind) * PAD, PAD), PAD)
            parts = value.astype(BF16).reshape(4, 2, BLOCK, PAD)
            for cc in range(2):
                GP[cc, block_row, :, :, lanes] = parts[:, cc]

        store(row, 1, grad_keys)
        store(row, 2, grad_values)

        @pl.when(row == 3)
        def _():
            for r in range(4):
                store(r, 0, GQ[r * TILE : (r + 1) * TILE])
            lanes = pl.ds(pl.multiple_of(h * 3 * PAD, PAD), 3 * PAD)
            send(
                GP.at[1 - c, :, :, :, lanes], GP2.at[:, :, :, lanes], s_gp, r_gp.at[h], seq=partner
            )

    arrived(W2, r_wd)
    for h in range(2):
        arrived(GP2.at[:, :, :, h * 3 * PAD : (h + 1) * 3 * PAD], r_gp.at[h])

    xr, xl, xo = (x + 1) % 4, (x + 3) % 4, (x + 2) % 4

    def lanes_of(n):
        return pl.ds(pl.multiple_of(n * NB, NB), NB)

    @pl.loop(0, NSTEPS)
    def _(n):
        lanes = lanes_of(n)
        mine = GP[c].reshape(512, 6 * PAD)
        other = GP2[...].reshape(512, 6 * PAD)
        part = dot(mine, Wp[:, :, lanes].reshape(6 * PAD, NB), NN)
        part = part + dot(other, W2[:, :, lanes].reshape(6 * PAD, NB), NN)
        part = part.reshape(4, 4, BLOCK, NB)
        PF[:, :, :, lanes] = part
        PB[:, :, lanes] = PF[:, xo, :, lanes].astype(BF16)
        send(PB.at[:, pl.ds(0, 16), lanes], R1L.at[:, :, lanes], s_r1, r_r1l.at[n], seq=right)
        send(PB.at[:, pl.ds(16, 16), lanes], R1R.at[:, :, lanes], s_r1, r_r1r.at[n], seq=left)

    @pl.loop(0, NSTEPS)
    def _(n):
        lanes = lanes_of(n)
        arrived(R1L.at[:, :, lanes], r_r1l.at[n])
        S2R[:, 0:16, lanes] = (
            PF[:, xr, 0:16, lanes] + R1L[:, :, lanes].astype(F32)
        ).astype(BF16)
        S2R[:, 16:32, lanes] = PF[:, xr, 16:32, lanes].astype(BF16)
        send(S2R.at[:, :, lanes], R2L.at[:, :, lanes], s_r2, r_r2l.at[n], seq=right)
        arrived(R1R.at[:, :, lanes], r_r1r.at[n])
        S2L[:, 16:32, lanes] = (
            PF[:, xl, 16:32, lanes] + R1R[:, :, lanes].astype(F32)
        ).astype(BF16)
        S2L[:, 0:16, lanes] = PF[:, xl, 0:16, lanes].astype(BF16)
        send(S2L.at[:, :, lanes], R2R.at[:, :, lanes], s_r2, r_r2r.at[n], seq=left)

    @pl.loop(0, NSTEPS)
    def _(n):
        lanes = lanes_of(n)
        arrived(R2L.at[:, :, lanes], r_r2l.at[n])
        arrived(R2R.at[:, :, lanes], r_r2r.at[n])
        total = PF[:, x, :, lanes] + R2L[:, :, lanes].astype(F32) + R2R[:, :, lanes].astype(F32)
        YS[:, :, lanes] = total.astype(BF16)
        for d in range(1, 4):
            send(
                YS.at[(y + d) % 4, :, lanes], YR.at[y, :, lanes], s_ry, r_ry.at[d - 1, n],
                seq=at((y + d) % 4, x, c),
            )

    YR[y] = YS[y]

    @pl.loop(0, NSTEPS)
    def _(n):
        for d in range(1, 4):
            arrived(YR.at[(y + d) % 4, :, lanes_of(n)], r_ry.at[3 - d, n])

    lane = lax.broadcasted_iota(jnp.int32, (8, PAD), 1)
    line = lax.broadcasted_iota(jnp.int32, (8, PAD), 0)

    def total_of(value):
        return jnp.sum(jnp.sum(value, axis=0, keepdims=True), axis=1, keepdims=True)

    sums = jnp.zeros((8, PAD), F32)
    for i in range(IMAGES):
        scaled = YR[i].astype(F32) * gain[...]
        unit = normed[i]
        first = jnp.mean(scaled, axis=-1, keepdims=True)
        second = jnp.mean(scaled * unit, axis=-1, keepdims=True)
        gradient = RES[i] + (scaled - first - unit * second) * inv[i][:, 0:1]
        RES[i] = gradient
        current = pert[i]
        for j, value in enumerate((gradient * gradient, current * gradient, current * current)):
            sums = jnp.where((line == i) & (lane == j), total_of(value), sums)
    SC[...] = sums
    SCR[s] = sums

    @pl.loop(1, SEQ)
    def _(d):
        send(SC, SCR.at[s], s_sc, r_sc, seq=(s + d) % SEQ)

    arrived(SCR.at[pl.ds(0, SEQ - 1)], r_sc)
    sums = jnp.sum(SCR[...], axis=0)

    for i in range(IMAGES):
        grad_square = sums[i : i + 1, 0:1]
        cross = sums[i : i + 1, 1:2]
        own = sums[i : i + 1, 2:3]
        factor = stp[z * IMAGES + i] * lax.rsqrt(grad_square + norm_epsilon)
        stepped_square = own + 2.0 * factor * cross + factor * factor * grad_square
        shrink = jnp.minimum(1.0, rad[z * IMAGES + i] * lax.rsqrt(stepped_square + norm_epsilon))
        out[i] = (pert[i] + factor * RES[i]) * shrink

    @pl.when(offset != 0)
    def _():
        for j in range(3):
            arrived(w_own.at[j], s_wz)

    for j in range(9):
        arrived(w_own.at[j], s_wy)
    arrived(HS.at[pl.ds(0, 3)], s_hy)
    arrived(H.at[0, :, :].reshape(8, BLOCK, WIDTH), s_hx)
    arrived(H.at[0, pl.ds(0, 2)].reshape(4, BLOCK, WIDTH), s_hx)
    arrived(H.at[pl.ds(0, 2)].reshape(16, BLOCK, WIDTH), s_hd)
    arrived(Wp, s_wd)
    for j in range(7):
        arrived(wo_own.at[0], s_wo)
        arrived(wo_own.at[0], s_wod)
    arrived(flat_or.at[pl.ds(0, 62)], s_oa)
    arrived(flat_go.at[pl.ds(0, 62)], s_ga)
    arrived(GP2, s_gp)
    arrived(PB, s_r1)
    arrived(S2R, s_r2)
    arrived(S2L, s_r2)
    arrived(YS.at[pl.ds(0, 3)], s_ry)
    arrived(SCR.at[pl.ds(0, SEQ - 1)], s_sc)


def on_device(patch_embed, perturbation, target, ln_gain, ln_bias, w_qkv, w_out, radius, step_size):
    vmem = pl.BlockSpec(memory_space=pltpu.VMEM)
    smem = pl.BlockSpec(memory_space=pltpu.SMEM)
    anywhere = pl.BlockSpec(memory_space=pl.ANY)
    dma = pltpu.SemaphoreType.DMA
    V = pltpu.VMEM
    scratch = [
        V((4, 4, 2, BLOCK, WIDTH), BF16),
        V((6, PAD, WIDTH), BF16),
        V((6, PAD, WIDTH), BF16),
        V((PLANES, 2, PAD, WIDTH), BF16),
        V((IMAGES, BLOCK, WIDTH), F32),
        V((IMAGES, BLOCK, PAD), F32),
        V((IMAGES, BLOCK, WIDTH), BF16),
        V((2, 1024, PAD), BF16),
        V((2, 1024, PAD), BF16),
        V((2, 1024, PAD), BF16),
        V((2, 4, 8, BLOCK, PAD), BF16),
        V((2, 4, 8, BLOCK, PAD), BF16),
        V((2, 8, 1024), F32),
        V((2, 4, 8, BLOCK, PAD), BF16),
        V((2, 32, BLOCK, PAD), BF16),
        V((1024, PAD), F32),
        V((2, 4, 4, BLOCK, 6 * PAD), BF16),
        V((4, 4, BLOCK, 6 * PAD), BF16),
        V((IMAGES, BLOCK, WIDTH), F32),
        V((4, 4, BLOCK, WIDTH), F32),
        V((4, BLOCK, WIDTH), BF16),
        V((4, 16, WIDTH), BF16),
        V((4, 16, WIDTH), BF16),
        V((4, BLOCK, WIDTH), BF16),
        V((4, BLOCK, WIDTH), BF16),
        V((4, BLOCK, WIDTH), BF16),
        V((4, BLOCK, WIDTH), BF16),
        V((4, BLOCK, WIDTH), BF16),
        V((4, BLOCK, WIDTH), BF16),
        V((8, PAD), F32),
        V((SEQ, 8, PAD), F32),
        dma, dma((3,)), dma, dma((3,)), dma((3,)), dma((3,)),
        dma, dma((3,)), dma, dma((4,)), dma((4,)), dma((4,)), dma((4,)),
        dma, dma((16,)),
        dma, dma((8,)), dma, dma((8,)), dma,
        dma, dma,
        dma, dma, dma, dma,
        dma, dma((2,)),
        dma, dma((NSTEPS,)), dma((NSTEPS,)),
        dma, dma((NSTEPS,)), dma((NSTEPS,)),
        dma, dma((3, NSTEPS)),
        dma, dma,
    ]
    return pl.pallas_call(
        kernel,
        out_shape=jax.ShapeDtypeStruct(perturbation.shape, F32),
        in_specs=[vmem, vmem, vmem, vmem, vmem, anywhere, anywhere, smem, smem],
        out_specs=vmem,
        scratch_shapes=scratch,
        compiler_params=pltpu.CompilerParams(
            collective_id=0, has_side_effects=True, vmem_limit_bytes=62 * 1024 * 1024
        ),
    )(
        patch_embed,
        perturbation,
        target,
        ln_gain.reshape(1, -1),
        ln_bias.reshape(1, -1),
        w_qkv.reshape(12, CHUNK, WIDTH),
        w_out,
        radius,
        step_size,
    )


def solution(mesh):
    placed = (
        P("head", "seq", None),
        P("head", "seq", None),
        P("head", "seq", None),
        P(),
        P(),
        P("head", None, None),
        P("head", None, None),
        P(),
        P(),
    )
    return jax.shard_map(
        on_device, mesh=mesh, in_specs=placed, out_specs=P("head", "seq", None), check_vma=False
    )
```

```python
import functools
import math

import jax
import jax.numpy as jnp
from jax import lax
from jax.experimental import pallas as pl
from jax.experimental.pallas import tpu as pltpu
from jax.sharding import PartitionSpec as P

norm_epsilon = 1e-06
layer_epsilon = 1e-06

F32 = jnp.float32
BF16 = jnp.bfloat16
NT = (((1,), (1,)), ((), ()))
NN = (((1,), (0,)), ((), ()))
TN = (((0,), (0,)), ((), ()))

IMAGES = 4
ROWS = 4
COLS = 4
PLANES = 8
SEQ = 32
BLOCK = 32
WIDTH = 1280
HD = 80
PAD = 128
CHUNK = 40
NB = 256
NSTEPS = WIDTH // NB
CHUNKS = 6
TILE = 256


def dot(a, b, dims):
    return lax.dot_general(a, b, dims, preferred_element_type=F32)


def shard_offset(x, c):
    other = 8 - x - 4 * (1 - (x + 3) // 4)
    return (1 - c) * x + c * other


def kernel(
    pe_in, pert_in, tgt_in, gain_in, bias_in, w_own, wo_own, rad_in, stp_in, grad_out, sums_out,
    pe, pert, tgt, gain, bias, rad, stp,
    H, RB, Wp, W2, WO, normed, inv, HS, Q, K, V, O, OR, LSE, DOT, GS, GO, GQ, GP, GP2,
    RES, RESB, PF, PB, R1L, R1R, S2L, S2R, R2L, R2R, YS, YR, SC, SCR,
    l_in, l_out, s_rb, r_rb, s_wz, r_wz, s_wy, r_wyl, r_wyr, r_wyy, s_hy, r_hy, s_hx, r_hxl, r_hxr, r_hxy, r_hxz,
    s_hd, r_hd, s_wo, r_wo, s_woy, r_wol, r_wor, r_woz, s_wod, r_wod, l_wo, s_wd, r_wd, s_oa, r_oa, s_ga, r_ga,
    s_gp, r_gp, s_r1, r_r1l, r_r1r, s_r2, r_r2l, r_r2r, s_ry, r_ry, s_sc, r_sc,
):
    s = lax.axis_index("seq")
    z = lax.axis_index("head")
    y = s // 8
    x = (s // 2) % 4
    c = s % 2
    k8 = s % 8

    def at(yy, xx, cc):
        return (yy * 4 + xx) * 2 + cc

    right = at(y, (x + 1) % 4, c)
    left = at(y, (x + 3) % 4, c)
    down = at((y + 1) % 4, x, c)
    up = at((y + 3) % 4, x, c)
    partner = at(y, x, 1 - c)

    def send(src, dst, ssem, rsem, **where):
        copy = pltpu.make_async_remote_copy(
            src_ref=src, dst_ref=dst, send_sem=ssem, recv_sem=rsem,
            device_id=where, device_id_type=pl.DeviceIdType.MESH,
        )
        copy.start()

    def arrived(ref, sem):
        pltpu.make_async_copy(ref, ref, sem).wait()

    loads = [
        pltpu.make_async_copy(src, dst, l_in.at[i])
        for i, (src, dst) in enumerate(
            ((pe_in, pe), (pert_in, pert), (tgt_in, tgt), (gain_in, gain), (bias_in, bias),
             (rad_in, rad), (stp_in, stp))
        )
    ]
    for load in loads:
        load.start()

    barrier = pltpu.get_barrier_semaphore()

    @pl.loop(1, SEQ)
    def _(d):
        pl.semaphore_signal(
            barrier, inc=1, device_id={"seq": (s + d) % SEQ}, device_id_type=pl.DeviceIdType.MESH
        )

    @pl.loop(1, PLANES)
    def _(d):
        pl.semaphore_signal(
            barrier, inc=1, device_id={"head": (z + d) % PLANES},
            device_id_type=pl.DeviceIdType.MESH,
        )

    own_wo = pltpu.make_async_copy(wo_own, WO.at[z, :, pl.ds(0, HD)], l_wo)
    own_wo.start()

    @pl.loop(0, 6)
    def _(t):
        Wp[t, HD:PAD, :] = jnp.zeros((PAD - HD, WIDTH), BF16)

    @pl.loop(0, 16)
    def _(t):
        WO[t // 2, t % 2, HD:PAD, :] = jnp.zeros((PAD - HD, WIDTH), BF16)

    def layer_norm(image):
        mixed = pe[image].astype(F32) + pert[image]
        rounded = mixed.astype(BF16).astype(F32)
        center = rounded - jnp.mean(rounded, axis=-1, keepdims=True)
        variance = jnp.mean(center * center, axis=-1, keepdims=True)
        inverse = lax.rsqrt(variance + layer_epsilon)
        unit = center * inverse
        normed[image] = unit
        inv[image] = jnp.broadcast_to(inverse, (BLOCK, PAD))
        RES[image] = mixed - tgt[image].astype(F32)
        return (unit * gain[...].reshape(1, WIDTH) + bias[...].reshape(1, WIDTH)).astype(BF16)

    for load in loads:
        load.wait()

    @pl.loop(1, ROWS)
    def _(d):
        image = (y + d) % 4
        HS[image] = layer_norm(image)

    H[y, x, c] = layer_norm(y)

    pl.semaphore_wait(barrier, SEQ - 1 + PLANES - 1)

    offset = shard_offset(x, c)
    target = (z + 8 - offset) % 8

    half_width = WIDTH // 2

    def chunk(yy, q):
        u = 3 * yy + q % 3
        rows = pl.ds(pl.multiple_of(CHUNK * (u % 2), 8), CHUNK)
        return Wp.at[u // 2, rows, pl.ds((q // 3) * half_width, half_width)]

    def source(q):
        return w_own.at[3 * y + q % 3, :, pl.ds((q // 3) * half_width, half_width)]

    between = {0: (0, 2), 1: (1, 6), 3: (2, 2), 4: (3, 6)}

    for q in range(CHUNKS):
        @pl.when(offset == 0)
        def _():
            pltpu.make_async_copy(source(q), chunk(y, q), r_wz.at[q]).start()

        if q in between:
            slot, hop = between[q]

            @pl.when(offset == 4)
            def _():
                send(source(q), RB.at[slot], s_wz, r_rb.at[slot], head=(z + hop) % 8)

            @pl.when((offset != 0) & (offset != 4))
            def _():
                send(source(q), chunk(y, q), s_wz, r_wz.at[q], head=target)
        else:
            @pl.when(offset != 0)
            def _():
                send(source(q), chunk(y, q), s_wz, r_wz.at[q], head=target)

    def pass_on(q):
        slot, hop = between[q]

        @pl.when(offset == 4)
        def _():
            arrived(RB.at[slot], r_rb.at[slot])
            send(RB.at[slot], chunk(y, q), s_rb, r_wz.at[q], head=(z + hop) % 8)

    @pl.loop(1, ROWS)
    def _(d):
        image = (y + d) % 4
        send(HS.at[image], H.at[y, x, c], s_hy, r_hy.at[d - 1], seq=at(image, x, c))

    def spread(d):
        yy = (y + d) % 4
        block = H.at[yy, x, c]
        send(block, block, s_hx, r_hxl.at[d], seq=right)
        send(block, block, s_hx, r_hxr.at[d], seq=left)
        send(block, block, s_hd, r_hd.at[d * 4], seq=partner)

    def relay(d):
        yy = (y + d) % 4
        from_left = H.at[yy, (x + 3) % 4, c]
        arrived(from_left, r_hxl.at[d])
        upper = H.at[yy, (x + 3) % 4, c, pl.ds(0, 16)]
        send(upper, upper, s_hx, r_hxy.at[d], seq=right)
        send(from_left, from_left, s_hd, r_hd.at[d * 4 + 1], seq=partner)
        from_right = H.at[yy, (x + 1) % 4, c]
        arrived(from_right, r_hxr.at[d])
        lower = H.at[yy, (x + 1) % 4, c, pl.ds(16, 16)]
        send(lower, lower, s_hx, r_hxz.at[d], seq=left)
        send(from_right, from_right, s_hd, r_hd.at[d * 4 + 2], seq=partner)

    def from_row(d):
        arrived(H.at[(y + d) % 4, x, c], r_hy.at[3 - d])
        spread(d)

    def round_column(j):
        arrived(chunk(y, j), r_wz.at[j])
        send(chunk(y, j), chunk(y, j), s_wy, r_wyl.at[j], seq=down)
        send(chunk(y, j), chunk(y, j), s_wy, r_wyr.at[j], seq=up)

    def ways(plane):
        odd = plane % 2
        place = odd * y + (1 - odd) * x
        return place, odd * down + (1 - odd) * right, odd * up + (1 - odd) * left

    def piece(ref, place, cc):
        rows = pl.ds(pl.multiple_of(CHUNK * (place % 2), 8), CHUNK)
        lanes = pl.ds(pl.multiple_of(cc * half_width, PAD), half_width)
        return ref.at[place // 2, rows, lanes]

    def half_shard(plane, cc):
        lanes = pl.ds(pl.multiple_of(cc * half_width, PAD), half_width)
        return WO.at[plane, :, pl.ds(0, HD), lanes]

    def wo_start():
        place, _, _ = ways(z)
        mine, there = piece(wo_own, place, c), piece(WO.at[z], place, c)
        send(mine, there, s_wo, r_wo.at[1], head=(z + 1) % 8)
        send(mine, there, s_wo, r_wo.at[7], head=(z + 7) % 8)

    def wo_chain(step):
        for d, ahead, there, last in ((step, 1, step + 1, 4), (8 - step, 7, 7 - step, 5)):
            if step == 4 and ahead == 7:
                continue
            plane = (z + 8 - d) % 8
            place, _, _ = ways(plane)
            got = piece(WO.at[plane], place, c)
            arrived(got, r_wo.at[d])
            if d != last:
                send(got, got, s_wo, r_wo.at[there], head=(z + ahead) % 8)

    def wo_first(d):
        plane = (z + 8 - d) % 8
        place, after, before = ways(plane)
        got = piece(WO.at[plane], place, c)
        send(got, got, s_woy, r_wol.at[d], seq=after)
        send(got, got, s_woy, r_wor.at[d], seq=before)

    def wo_second(d):
        plane = (z + 8 - d) % 8
        place, after, before = ways(plane)
        shard = WO.at[plane]
        lower, upper = piece(shard, (place + 3) % 4, c), piece(shard, (place + 1) % 4, c)
        arrived(lower, r_wol.at[d])
        arrived(upper, r_wor.at[d])
        turn = (plane // 2) % 2

        @pl.when(turn == 0)
        def _():
            send(lower, lower, s_woy, r_woz.at[d], seq=after)

        @pl.when(turn == 1)
        def _():
            send(upper, upper, s_woy, r_woz.at[d], seq=before)

    def wo_third(d):
        plane = (z + 8 - d) % 8
        place, _, _ = ways(plane)
        arrived(piece(WO.at[plane], (place + 2) % 4, c), r_woz.at[d])
        got = half_shard(plane, c)
        send(got, got, s_wod, r_wod.at[d], seq=partner)

    yu, yd, yo = (y + 3) % 4, (y + 1) % 4, (y + 2) % 4

    def relay_column(q):
        arrived(chunk(yu, q), r_wyl.at[q])
        arrived(chunk(yd, q), r_wyr.at[q])
        if q % 2 == 0:
            send(chunk(yu, q), chunk(yu, q), s_wy, r_wyy.at[q], seq=down)
        else:
            send(chunk(yd, q), chunk(yd, q), s_wy, r_wyy.at[q], seq=up)

    def far_column(d):
        yy, xx = (y + d) % 4, (x + 2) % 4
        arrived(H.at[yy, xx, c, pl.ds(0, 16)], r_hxy.at[d])
        arrived(H.at[yy, xx, c, pl.ds(16, 16)], r_hxz.at[d])
        send(H.at[yy, xx, c], H.at[yy, xx, c], s_hd, r_hd.at[d * 4 + 3], seq=partner)

    spread(0)
    wo_start()
    from_row(1)
    relay(0)
    from_row(3)
    pass_on(0)
    pass_on(1)
    from_row(2)
    round_column(0)
    round_column(1)
    relay(1)
    round_column(2)
    relay_column(0)
    relay(3)
    wo_chain(1)
    pass_on(3)
    pass_on(4)
    relay_column(1)
    relay(2)
    round_column(3)
    relay_column(2)
    round_column(4)
    far_column(0)
    round_column(5)
    relay_column(3)
    wo_chain(2)
    far_column(1)
    relay_column(4)
    far_column(3)
    relay_column(5)
    far_column(2)

    for q in range(CHUNKS):
        arrived(chunk(yo, q), r_wyy.at[q])

    send(Wp, W2, s_wd, r_wd, seq=partner)
    wo_chain(3)
    for d in (1, 7, 2, 6):
        wo_first(d)

    @pl.loop(0, ROWS)
    def _(d):
        yy = (y + d) % 4
        arrived(H.at[yy, x, 1 - c], r_hd.at[d * 4])
        arrived(H.at[yy, (x + 3) % 4, 1 - c], r_hd.at[d * 4 + 1])
        arrived(H.at[yy, (x + 1) % 4, 1 - c], r_hd.at[d * 4 + 2])
        arrived(H.at[yy, (x + 2) % 4, 1 - c], r_hd.at[d * 4 + 3])
        rows = pl.ds(pl.multiple_of(yy * 256, 256), 256)
        tokens = H[yy].reshape(256, WIDTH)
        packed = dot(tokens, Wp[...].reshape(6 * PAD, WIDTH), NT).astype(BF16)
        for h in range(2):
            Q[h, rows] = packed[:, (3 * h) * PAD : (3 * h + 1) * PAD]
            K[h, rows] = packed[:, (3 * h + 1) * PAD : (3 * h + 2) * PAD]
            V[h, rows] = packed[:, (3 * h + 2) * PAD : (3 * h + 3) * PAD]

    scale = 1.0 / math.sqrt(HD)

    wo_chain(4)
    for d in (3, 5, 4):
        wo_first(d)

    @pl.loop(0, 4)
    def _(step):
        row = (y + 3 - step) % 4

        @pl.when(step == 1)
        def _():
            for d in (1, 7, 2, 6):
                wo_second(d)

        @pl.when(step == 2)
        def _():
            for d in (3, 5, 4):
                wo_second(d)

        @pl.when(step == 3)
        def _():
            for d in (1, 7, 2, 6):
                wo_third(d)

        rows = pl.ds(pl.multiple_of(row * TILE, TILE), TILE)
        for h in range(2):
            scores = dot(Q[h, rows], K[h], NT) * scale
            top = jnp.max(scores, axis=-1, keepdims=True)
            grown = jnp.exp(scores - top)
            total = jnp.sum(grown, axis=-1, keepdims=True)
            weights = (grown * (1.0 / total)).astype(BF16)
            part = dot(weights, V[h], NN).astype(BF16)
            O[h, row] = part.reshape(8, BLOCK, PAD)
            column = jnp.broadcast_to(top + jnp.log(total), (TILE, PAD))
            LSE[h, :, rows] = jnp.transpose(column)[0:8]

        @pl.loop(0, 8)
        def _(turn):
            k = (k8 + 7 - turn) % 8
            dest = row * 8 + k

            @pl.when(dest != s)
            def _():
                for h in range(2):
                    send(O.at[h, row, k], OR.at[h, y, k8], s_oa, r_oa, seq=dest)

    for h in range(2):
        OR[h, y, k8] = O[h, y, k8]

    for d in (3, 5, 4):
        wo_third(d)
    own_wo.wait()
    for d in range(1, PLANES):
        arrived(half_shard((z + 8 - d) % 8, 1 - c), r_wod.at[d])

    flat_or = OR.reshape(64, BLOCK, PAD)
    arrived(flat_or.at[pl.ds(0, 62)], r_oa)

    @pl.loop(0, 8)
    def _(k):
        kk = (z + shard_offset((k // 2), k % 2)) % 8
        heads = jnp.concatenate([OR[h, :, k].reshape(128, PAD) for h in range(2)], axis=-1)
        branch = dot(heads, WO[kk].reshape(2 * PAD, WIDTH), NN)
        RES[...] += branch.reshape(IMAGES, BLOCK, WIDTH)

    RESB[...] = RES[...].reshape(128, WIDTH).astype(BF16)

    @pl.loop(0, 8)
    def _(turn):
        k = ((x + 3 - turn // 2) % 4) * 2 + turn % 2
        kk = (z + shard_offset((k // 2), k % 2)) % 8
        back = dot(RESB[...], WO[kk].reshape(2 * PAD, WIDTH), NT).astype(BF16)
        for h in range(2):
            GS[h, :, k] = back[:, h * PAD : (h + 1) * PAD].reshape(IMAGES, BLOCK, PAD)

        @pl.loop(0, IMAGES)
        def _(turn):
            i = (y + 3 - turn) % 4
            dest = i * 8 + k

            @pl.when(dest != s)
            def _():
                for h in range(2):
                    send(GS.at[h, i, k], GO.at[h, s], s_ga, r_ga, seq=dest)

    for h in range(2):
        GO[h, s] = GS[h, y, k8]

    flat_go = GO.reshape(64, BLOCK, PAD)
    arrived(flat_go.at[pl.ds(0, 62)], r_ga)

    for h in range(2):
        products = GO[h].reshape(1024, PAD).astype(F32) * O[h].reshape(1024, PAD).astype(F32)
        DOT[h] = jnp.broadcast_to(
            jnp.sum(jnp.transpose(products), axis=0, keepdims=True), (8, 1024)
        )

    def store(block_row, h, kind, value):
        parts = value.astype(BF16).reshape(4, 2, BLOCK, PAD)
        t = h * 3 + kind
        for cc in range(2):
            GP[cc, block_row, :, :, t * PAD : (t + 1) * PAD] = parts[:, cc]

    @pl.loop(0, 4)
    def _(row):
        rows = pl.ds(pl.multiple_of(row * TILE, TILE), TILE)
        for h in range(2):
            queries = Q[h]
            grads = GO[h].reshape(1024, PAD)
            scores = dot(K[h, rows], queries, NT) * scale
            weights = jnp.exp(scores - LSE[h, 0:1])
            grad_values = dot(weights.astype(BF16), grads, NN)
            grad_weights = dot(V[h, rows], grads, NT)
            grad_scores = (weights * (grad_weights - DOT[h, 0:1]) * scale).astype(BF16)
            grad_keys = dot(grad_scores, queries, NN)
            grad_query = dot(grad_scores, K[h, rows], TN)

            @pl.when(row == 0)
            def _():
                GQ[h] = grad_query

            @pl.when(row != 0)
            def _():
                GQ[h] += grad_query

            store(row, h, 1, grad_keys)
            store(row, h, 2, grad_values)

        for h in range(2):
            lanes = pl.ds((h * 3 + 1) * PAD, 2 * PAD)
            send(
                GP.at[1 - c, row, :, :, lanes], GP2.at[row, :, :, lanes], s_gp, r_gp.at[h, row],
                seq=partner,
            )

    for h in range(2):
        for r in range(4):
            store(r, h, 0, GQ[h, r * TILE : (r + 1) * TILE])
        lanes = pl.ds(h * 3 * PAD, PAD)
        send(GP.at[1 - c, :, :, :, lanes], GP2.at[:, :, :, lanes], s_gp, r_gp.at[h, 4], seq=partner)

    arrived(W2, r_wd)
    for h in range(2):
        for r in range(4):
            arrived(GP2.at[r, :, :, pl.ds((h * 3 + 1) * PAD, 2 * PAD)], r_gp.at[h, r])
        arrived(GP2.at[:, :, :, pl.ds(h * 3 * PAD, PAD)], r_gp.at[h, 4])

    xr, xl, xo = (x + 1) % 4, (x + 3) % 4, (x + 2) % 4

    def lanes_of(n):
        return pl.ds(pl.multiple_of(n * NB, NB), NB)

    @pl.loop(0, NSTEPS)
    def _(n):
        lanes = lanes_of(n)
        mine = GP[c].reshape(512, 6 * PAD)
        other = GP2[...].reshape(512, 6 * PAD)
        part = dot(mine, Wp[:, :, lanes].reshape(6 * PAD, NB), NN)
        part = part + dot(other, W2[:, :, lanes].reshape(6 * PAD, NB), NN)
        part = part.reshape(4, 4, BLOCK, NB)
        PF[:, :, :, lanes] = part
        PB[:, :, lanes] = PF[:, xo, :, lanes].astype(BF16)
        send(PB.at[:, pl.ds(0, 16), lanes], R1L.at[:, :, lanes], s_r1, r_r1l.at[n], seq=right)
        send(PB.at[:, pl.ds(16, 16), lanes], R1R.at[:, :, lanes], s_r1, r_r1r.at[n], seq=left)

    @pl.loop(0, NSTEPS)
    def _(n):
        lanes = lanes_of(n)
        arrived(R1L.at[:, :, lanes], r_r1l.at[n])
        S2R[:, 0:16, lanes] = (
            PF[:, xr, 0:16, lanes] + R1L[:, :, lanes].astype(F32)
        ).astype(BF16)
        S2R[:, 16:32, lanes] = PF[:, xr, 16:32, lanes].astype(BF16)
        send(S2R.at[:, :, lanes], R2L.at[:, :, lanes], s_r2, r_r2l.at[n], seq=right)
        arrived(R1R.at[:, :, lanes], r_r1r.at[n])
        S2L[:, 16:32, lanes] = (
            PF[:, xl, 16:32, lanes] + R1R[:, :, lanes].astype(F32)
        ).astype(BF16)
        S2L[:, 0:16, lanes] = PF[:, xl, 0:16, lanes].astype(BF16)
        send(S2L.at[:, :, lanes], R2R.at[:, :, lanes], s_r2, r_r2r.at[n], seq=left)

    @pl.loop(0, NSTEPS)
    def _(n):
        lanes = lanes_of(n)
        arrived(R2L.at[:, :, lanes], r_r2l.at[n])
        arrived(R2R.at[:, :, lanes], r_r2r.at[n])
        total = PF[:, x, :, lanes] + R2L[:, :, lanes].astype(F32) + R2R[:, :, lanes].astype(F32)
        YS[:, :, lanes] = total.astype(BF16)
        for d in range(1, 4):
            send(
                YS.at[(y + d) % 4, :, lanes], YR.at[y, :, lanes], s_ry, r_ry.at[d - 1, n],
                seq=at((y + d) % 4, x, c),
            )

    YR[y] = YS[y]

    @pl.loop(0, NSTEPS)
    def _(n):
        for d in range(1, 4):
            arrived(YR.at[(y + d) % 4, :, lanes_of(n)], r_ry.at[3 - d, n])

    lane = lax.broadcasted_iota(jnp.int32, (8, PAD), 1)
    line = lax.broadcasted_iota(jnp.int32, (8, PAD), 0)

    def total_of(value):
        return jnp.sum(jnp.sum(value, axis=0, keepdims=True), axis=1, keepdims=True)

    sums = jnp.zeros((8, PAD), F32)
    for i in range(IMAGES):
        scaled = YR[i].astype(F32) * gain[...].reshape(1, WIDTH)
        unit = normed[i]
        first = jnp.mean(scaled, axis=-1, keepdims=True)
        second = jnp.mean(scaled * unit, axis=-1, keepdims=True)
        gradient = RES[i] + (scaled - first - unit * second) * inv[i][:, 0:1]
        RES[i] = gradient
        pltpu.make_async_copy(RES.at[i], grad_out.at[i], l_out.at[i]).start()
        current = pert[i]
        for j, value in enumerate((gradient * gradient, current * gradient, current * current)):
            sums = jnp.where((line == i) & (lane == j), total_of(value), sums)
    SC[...] = sums
    SCR[s] = sums

    @pl.loop(1, SEQ)
    def _(d):
        send(SC, SCR.at[s], s_sc, r_sc, seq=(s + d) % SEQ)

    arrived(SCR.at[pl.ds(0, SEQ - 1)], r_sc)
    sums = jnp.sum(SCR[...], axis=0)
    column = lax.broadcasted_iota(jnp.int32, (8, 1), 0)
    step_of, radius_of = jnp.ones((8, 1), F32), jnp.ones((8, 1), F32)
    for i in range(IMAGES):
        step_of = jnp.where(column == i, stp[z * IMAGES + i], step_of)
        radius_of = jnp.where(column == i, rad[z * IMAGES + i], radius_of)
    grad_square, cross, own = sums[:, 0:1], sums[:, 1:2], sums[:, 2:3]
    factor = step_of / jnp.sqrt(grad_square + norm_epsilon)
    stepped_square = own + 2.0 * factor * cross + factor * factor * grad_square
    shrink = jnp.minimum(1.0, radius_of / jnp.sqrt(stepped_square + norm_epsilon))
    sums_out[...] = jnp.where(lane == 0, shrink, factor * shrink)
    for i in range(IMAGES):
        pltpu.make_async_copy(RES.at[i], grad_out.at[i], l_out.at[i]).wait()

    @pl.when(offset != 0)
    def _():
        for q in range(CHUNKS):
            arrived(source(q), s_wz)

    @pl.when(offset == 4)
    def _():
        arrived(RB, s_rb)

    for q in range(CHUNKS):
        for _ in range(3):
            arrived(source(q), s_wy)
    arrived(HS.at[pl.ds(0, 3)], s_hy)
    arrived(H.at[0, :, :].reshape(8, BLOCK, WIDTH), s_hx)
    arrived(H.at[0, pl.ds(0, 2)].reshape(4, BLOCK, WIDTH), s_hx)
    arrived(H.at[pl.ds(0, 2)].reshape(16, BLOCK, WIDTH), s_hd)
    arrived(Wp, s_wd)
    for d in range(1, PLANES):
        arrived(piece(wo_own, y, c), s_wo)
        for _ in range(3):
            arrived(piece(wo_own, y, c), s_woy)
        arrived(half_shard(z, c), s_wod)
    arrived(flat_or.at[pl.ds(0, 62)], s_oa)
    arrived(flat_go.at[pl.ds(0, 62)], s_ga)
    arrived(GP2, s_gp)
    arrived(PB, s_r1)
    arrived(S2R, s_r2)
    arrived(S2L, s_r2)
    arrived(YS.at[pl.ds(0, 3)], s_ry)
    arrived(SCR.at[pl.ds(0, SEQ - 1)], s_sc)


def on_device(patch_embed, perturbation, target, ln_gain, ln_bias, w_qkv, w_out, radius, step_size):
    vmem = pl.BlockSpec(memory_space=pltpu.VMEM)
    anywhere = pl.BlockSpec(memory_space=pl.ANY)
    dma = pltpu.SemaphoreType.DMA
    V = pltpu.VMEM
    scratch = [
        V(patch_embed.shape, BF16),
        V(perturbation.shape, F32),
        V(target.shape, BF16),
        V(ln_gain.shape, F32),
        V(ln_bias.shape, F32),
        pltpu.SMEM(radius.shape, F32),
        pltpu.SMEM(step_size.shape, F32),
        V((4, 4, 2, BLOCK, WIDTH), BF16),
        V((4, CHUNK, WIDTH // 2), BF16),
        V((6, PAD, WIDTH), BF16),
        V((6, PAD, WIDTH), BF16),
        V((PLANES, 2, PAD, WIDTH), BF16),
        V((IMAGES, BLOCK, WIDTH), F32),
        V((IMAGES, BLOCK, PAD), F32),
        V((IMAGES, BLOCK, WIDTH), BF16),
        V((2, 1024, PAD), BF16),
        V((2, 1024, PAD), BF16),
        V((2, 1024, PAD), BF16),
        V((2, 4, 8, BLOCK, PAD), BF16),
        V((2, 4, 8, BLOCK, PAD), BF16),
        V((2, 8, 1024), F32),
        V((2, 8, 1024), F32),
        V((2, 4, 8, BLOCK, PAD), BF16),
        V((2, 32, BLOCK, PAD), BF16),
        V((2, 1024, PAD), F32),
        V((2, 4, 4, BLOCK, 6 * PAD), BF16),
        V((4, 4, BLOCK, 6 * PAD), BF16),
        V((IMAGES, BLOCK, WIDTH), F32),
        V((IMAGES * BLOCK, WIDTH), BF16),
        V((4, 4, BLOCK, WIDTH), F32),
        V((4, BLOCK, WIDTH), BF16),
        V((4, 16, WIDTH), BF16),
        V((4, 16, WIDTH), BF16),
        V((4, BLOCK, WIDTH), BF16),
        V((4, BLOCK, WIDTH), BF16),
        V((4, BLOCK, WIDTH), BF16),
        V((4, BLOCK, WIDTH), BF16),
        V((4, BLOCK, WIDTH), BF16),
        V((4, BLOCK, WIDTH), BF16),
        V((8, PAD), F32),
        V((SEQ, 8, PAD), F32),
        dma((7,)), dma((IMAGES,)), dma, dma((4,)),
        dma, dma((CHUNKS,)), dma, dma((CHUNKS,)), dma((CHUNKS,)), dma((CHUNKS,)),
        dma, dma((3,)), dma, dma((4,)), dma((4,)), dma((4,)), dma((4,)),
        dma, dma((16,)),
        dma, dma((8,)), dma, dma((8,)), dma((8,)), dma((8,)), dma, dma((8,)), dma,
        dma, dma,
        dma, dma, dma, dma,
        dma, dma((2, 5)),
        dma, dma((NSTEPS,)), dma((NSTEPS,)),
        dma, dma((NSTEPS,)), dma((NSTEPS,)),
        dma, dma((3, NSTEPS)),
        dma, dma,
    ]
    gradient, sums = pl.pallas_call(
        kernel,
        out_shape=(
            jax.ShapeDtypeStruct(perturbation.shape, F32),
            jax.ShapeDtypeStruct((8, PAD), F32),
        ),
        in_specs=[anywhere] * 9,
        out_specs=(anywhere, vmem),
        scratch_shapes=scratch,
        compiler_params=pltpu.CompilerParams(
            collective_id=0, has_side_effects=True, vmem_limit_bytes=62 * 1024 * 1024
        ),
    )(
        patch_embed,
        perturbation,
        target,
        ln_gain,
        ln_bias,
        w_qkv.reshape(12, CHUNK, WIDTH),
        w_out,
        radius,
        step_size,
    )
    shrink, factor = sums[:IMAGES, 0:1, None], sums[:IMAGES, 1:2, None]
    return perturbation * shrink + factor * gradient


def solution(mesh):
    placed = (
        P("head", "seq", None),
        P("head", "seq", None),
        P("head", "seq", None),
        P(),
        P(),
        P("head", None, None),
        P("head", None, None),
        P(),
        P(),
    )
    return jax.shard_map(
        on_device, mesh=mesh, in_specs=placed, out_specs=P("head", "seq", None), check_vma=False
    )
```

```python
import functools
import math

import jax
import jax.numpy as jnp
from jax import lax
from jax.experimental import pallas as pl
from jax.experimental.pallas import tpu as pltpu
from jax.sharding import PartitionSpec as P

norm_epsilon = 1e-06
layer_epsilon = 1e-06

F32 = jnp.float32
BF16 = jnp.bfloat16
NT = (((1,), (1,)), ((), ()))
NN = (((1,), (0,)), ((), ()))
TN = (((0,), (0,)), ((), ()))

IMAGES = 4
ROWS = 4
COLS = 4
PLANES = 8
SEQ = 32
BLOCK = 32
WIDTH = 1280
HD = 80
PAD = 128
CHUNK = 40
NB = 256
NSTEPS = WIDTH // NB
CHUNKS = 6
TILE = 256


def dot(a, b, dims):
    return lax.dot_general(a, b, dims, preferred_element_type=F32)


def shard_offset(x, c):
    other = 8 - x - 4 * (1 - (x + 3) // 4)
    return (1 - c) * x + c * other


def kernel(
    pe_in, pert_in, tgt_in, gain_in, bias_in, w_own, wo_own, rad_in, stp_in, grad_out, shrink_out, factor_out,
    pe, pert, tgt, gain, bias, rad, stp,
    H, RB, Wp, W2, WO, normed, inv, HS, Q, K, V, O, OR, LSE, DOT, GS, GO, GQ, GP, GP2,
    RES, RESB, PF, PB, R1L, R1R, S2L, S2R, R2L, R2R, YS, YR, SC, SCR,
    l_in, l_out, s_rb, r_rb, s_wz, r_wz, s_wy, r_wyl, r_wyr, r_wyy, s_hy, r_hy, s_hx, r_hxl, r_hxr, r_hxy, r_hxz,
    s_hd, r_hd, s_wo, r_wo, r_wof, s_woy, r_wol, r_wor, r_woz, s_wod, r_wod, l_wo, s_wd, r_wd, s_oa, r_oa, s_ga, r_ga,
    s_gp, r_gp, s_r1, r_r1l, r_r1r, s_r2, r_r2l, r_r2r, s_ry, r_ry, s_sc, r_sc,
):
    s = lax.axis_index("seq")
    z = lax.axis_index("head")
    y = s // 8
    x = (s // 2) % 4
    c = s % 2
    k8 = s % 8

    def at(yy, xx, cc):
        return (yy * 4 + xx) * 2 + cc

    right = at(y, (x + 1) % 4, c)
    left = at(y, (x + 3) % 4, c)
    down = at((y + 1) % 4, x, c)
    up = at((y + 3) % 4, x, c)
    partner = at(y, x, 1 - c)

    def send(src, dst, ssem, rsem, **where):
        copy = pltpu.make_async_remote_copy(
            src_ref=src, dst_ref=dst, send_sem=ssem, recv_sem=rsem,
            device_id=where, device_id_type=pl.DeviceIdType.MESH,
        )
        copy.start()

    def arrived(ref, sem):
        pltpu.make_async_copy(ref, ref, sem).wait()

    loads = [
        pltpu.make_async_copy(src, dst, l_in.at[i])
        for i, (src, dst) in enumerate(
            ((pe_in, pe), (pert_in, pert), (gain_in, gain), (bias_in, bias), (tgt_in, tgt),
             (rad_in, rad), (stp_in, stp))
        )
    ]
    for load in loads:
        load.start()

    barrier = pltpu.get_barrier_semaphore()

    for d in range(1, SEQ):
        pl.semaphore_signal(
            barrier, inc=1, device_id={"seq": (s + d) % SEQ}, device_id_type=pl.DeviceIdType.MESH
        )
    for d in range(1, PLANES):
        pl.semaphore_signal(
            barrier, inc=1, device_id={"head": (z + d) % PLANES},
            device_id_type=pl.DeviceIdType.MESH,
        )

    own_wo = pltpu.make_async_copy(wo_own, WO.at[z, :, pl.ds(0, HD)], l_wo)
    own_wo.start()

    def normalize(image):
        mixed = pe[image].astype(F32) + pert[image]
        rounded = mixed.astype(BF16).astype(F32)
        center = rounded - jnp.mean(rounded, axis=-1, keepdims=True)
        variance = jnp.mean(center * center, axis=-1, keepdims=True)
        inverse = lax.rsqrt(variance + layer_epsilon)
        return mixed, center * inverse, inverse

    def layer_norm(image):
        _, unit, _ = normalize(image)
        return (unit * gain[...].reshape(1, WIDTH) + bias[...].reshape(1, WIDTH)).astype(BF16)

    for load in loads[:4]:
        load.wait()

    @pl.loop(1, ROWS)
    def _(d):
        image = (y + d) % 4
        HS[image] = layer_norm(image)

    H[y, x, c] = layer_norm(y)

    pl.semaphore_wait(barrier, SEQ - 1 + PLANES - 1)

    offset = shard_offset(x, c)
    target = (z + 8 - offset) % 8

    half_width = WIDTH // 2

    def ways(plane):
        odd = plane % 2
        place = odd * y + (1 - odd) * x
        return place, odd * down + (1 - odd) * right, odd * up + (1 - odd) * left

    def piece(ref, place, cc):
        rows = pl.ds(pl.multiple_of(CHUNK * (place % 2), 8), CHUNK)
        lanes = pl.ds(pl.multiple_of(cc * half_width, PAD), half_width)
        return ref.at[place // 2, rows, lanes]

    def half_shard(plane, cc):
        lanes = pl.ds(pl.multiple_of(cc * half_width, PAD), half_width)
        return WO.at[plane, :, pl.ds(0, HD), lanes]

    place, _, _ = ways(z)
    for d in (1, 7):
        send(piece(wo_own, place, c), piece(WO.at[z], place, c), s_wo, r_wo.at[d], head=(z + d) % 8)

    def chunk(yy, q):
        u = 3 * yy + q % 3
        rows = pl.ds(pl.multiple_of(CHUNK * (u % 2), 8), CHUNK)
        return Wp.at[u // 2, rows, pl.ds((q // 3) * half_width, half_width)]

    def source(q):
        return w_own.at[3 * y + q % 3, :, pl.ds((q // 3) * half_width, half_width)]

    between = {0: (0, 2), 1: (1, 6), 3: (2, 2), 4: (3, 6)}

    for q in range(CHUNKS):
        @pl.when(offset == 0)
        def _():
            pltpu.make_async_copy(source(q), chunk(y, q), r_wz.at[q]).start()

        if q in between:
            slot, hop = between[q]

            @pl.when(offset == 4)
            def _():
                send(source(q), RB.at[slot], s_wz, r_rb.at[slot], head=(z + hop) % 8)

            @pl.when((offset != 0) & (offset != 4))
            def _():
                send(source(q), chunk(y, q), s_wz, r_wz.at[q], head=target)
        else:
            @pl.when(offset != 0)
            def _():
                send(source(q), chunk(y, q), s_wz, r_wz.at[q], head=target)

    def pass_on(q):
        slot, hop = between[q]

        @pl.when(offset == 4)
        def _():
            arrived(RB.at[slot], r_rb.at[slot])
            send(RB.at[slot], chunk(y, q), s_rb, r_wz.at[q], head=(z + hop) % 8)

    @pl.loop(1, ROWS)
    def _(d):
        image = (y + d) % 4
        send(HS.at[image], H.at[y, x, c], s_hy, r_hy.at[d - 1], seq=at(image, x, c))

    def spread(d):
        yy = (y + d) % 4
        block = H.at[yy, x, c]
        send(block, block, s_hx, r_hxl.at[d], seq=right)
        send(block, block, s_hx, r_hxr.at[d], seq=left)
        send(block, block, s_hd, r_hd.at[d * 4], seq=partner)

    def relay(d):
        yy = (y + d) % 4
        from_left = H.at[yy, (x + 3) % 4, c]
        arrived(from_left, r_hxl.at[d])
        upper = H.at[yy, (x + 3) % 4, c, pl.ds(0, 16)]
        send(upper, upper, s_hx, r_hxy.at[d], seq=right)
        send(from_left, from_left, s_hd, r_hd.at[d * 4 + 1], seq=partner)
        from_right = H.at[yy, (x + 1) % 4, c]
        arrived(from_right, r_hxr.at[d])
        lower = H.at[yy, (x + 1) % 4, c, pl.ds(16, 16)]
        send(lower, lower, s_hx, r_hxz.at[d], seq=left)
        send(from_right, from_right, s_hd, r_hd.at[d * 4 + 2], seq=partner)

    def from_row(d):
        arrived(H.at[(y + d) % 4, x, c], r_hy.at[3 - d])
        spread(d)

    def round_column(j):
        arrived(chunk(y, j), r_wz.at[j])
        send(chunk(y, j), chunk(y, j), s_wy, r_wyl.at[j], seq=down)
        send(chunk(y, j), chunk(y, j), s_wy, r_wyr.at[j], seq=up)

    def wo_chain(step):
        for d, ahead, there, last in ((step, 1, step + 1, 4), (8 - step, 7, 7 - step, 5)):
            if step == 4 and ahead == 7:
                continue
            plane = (z + 8 - d) % 8
            place, _, _ = ways(plane)
            got = piece(WO.at[plane], place, c)
            arrived(got, r_wo.at[d])
            if d != last:
                send(got, got, s_wo, r_wo.at[there], head=(z + ahead) % 8)

    def wo_give():
        place, _, _ = ways(z)
        for i, d in enumerate((1, 7)):
            for part in range(3):
                spot = (place + 1 + part) % 4
                send(
                    piece(wo_own, spot, c), piece(WO.at[z], spot, c), s_wo, r_wof.at[i, part],
                    head=(z + d) % 8,
                )

    def wo_near():
        for i, d in enumerate((1, 7)):
            plane = (z + 8 - d) % 8
            place, _, _ = ways(plane)
            for part in range(3):
                arrived(piece(WO.at[plane], (place + 1 + part) % 4, c), r_wof.at[i, part])
            send(half_shard(plane, c), half_shard(plane, c), s_wod, r_wod.at[d], seq=partner)

    def wo_first(d):
        plane = (z + 8 - d) % 8
        place, after, before = ways(plane)
        got = piece(WO.at[plane], place, c)
        send(got, got, s_woy, r_wol.at[d], seq=after)
        send(got, got, s_woy, r_wor.at[d], seq=before)
        send(got, got, s_wod, r_wod.at[d], seq=partner)

    def wo_second(d):
        plane = (z + 8 - d) % 8
        place, after, before = ways(plane)
        shard = WO.at[plane]
        lower, upper = piece(shard, (place + 3) % 4, c), piece(shard, (place + 1) % 4, c)
        arrived(lower, r_wol.at[d])
        arrived(upper, r_wor.at[d])
        send(lower, lower, s_wod, r_wod.at[d], seq=partner)
        send(upper, upper, s_wod, r_wod.at[d], seq=partner)
        turn = (plane // 2) % 2

        @pl.when(turn == 0)
        def _():
            send(lower, lower, s_woy, r_woz.at[d], seq=after)

        @pl.when(turn == 1)
        def _():
            send(upper, upper, s_woy, r_woz.at[d], seq=before)

    def wo_third(d):
        plane = (z + 8 - d) % 8
        place, _, _ = ways(plane)
        got = piece(WO.at[plane], (place + 2) % 4, c)
        arrived(got, r_woz.at[d])
        send(got, got, s_wod, r_wod.at[d], seq=partner)

    yu, yd, yo = (y + 3) % 4, (y + 1) % 4, (y + 2) % 4

    def relay_column(q):
        arrived(chunk(yu, q), r_wyl.at[q])
        arrived(chunk(yd, q), r_wyr.at[q])
        if q % 2 == 0:
            send(chunk(yu, q), chunk(yu, q), s_wy, r_wyy.at[q], seq=down)
        else:
            send(chunk(yd, q), chunk(yd, q), s_wy, r_wyy.at[q], seq=up)

    def far_column(d):
        yy, xx = (y + d) % 4, (x + 2) % 4
        arrived(H.at[yy, xx, c, pl.ds(0, 16)], r_hxy.at[d])
        arrived(H.at[yy, xx, c, pl.ds(16, 16)], r_hxz.at[d])
        send(H.at[yy, xx, c], H.at[yy, xx, c], s_hd, r_hd.at[d * 4 + 3], seq=partner)

    spread(0)

    @pl.loop(0, 6)
    def _(t):
        Wp[t, HD:PAD, :] = jnp.zeros((PAD - HD, WIDTH), BF16)

    @pl.loop(0, 16)
    def _(t):
        WO[t // 2, t % 2, HD:PAD, :] = jnp.zeros((PAD - HD, WIDTH), BF16)

    for load in loads[4:]:
        load.wait()

    @pl.loop(0, IMAGES)
    def _(image):
        mixed, unit, inverse = normalize(image)
        normed[image] = unit
        inv[image] = jnp.broadcast_to(inverse, (BLOCK, PAD))
        RES[image] = mixed - tgt[image].astype(F32)

    from_row(1)
    relay(0)
    wo_chain(1)
    from_row(3)
    pass_on(0)
    pass_on(1)
    from_row(2)
    round_column(0)
    round_column(1)
    pass_on(3)
    pass_on(4)
    relay(1)
    round_column(2)
    relay_column(0)
    relay(3)
    wo_chain(2)
    relay_column(1)
    relay(2)
    round_column(3)
    relay_column(2)
    round_column(4)
    far_column(0)
    round_column(5)
    wo_give()
    relay_column(3)
    wo_chain(3)
    wo_first(2)
    wo_first(6)
    far_column(1)
    relay_column(4)
    far_column(3)
    relay_column(5)
    far_column(2)

    for q in range(CHUNKS):
        arrived(chunk(yo, q), r_wyy.at[q])

    send(Wp, W2, s_wd, r_wd, seq=partner)
    wo_chain(4)
    for d in (3, 5, 4):
        wo_first(d)

    @pl.loop(0, ROWS)
    def _(d):
        yy = (y + d) % 4
        arrived(H.at[yy, x, 1 - c], r_hd.at[d * 4])
        arrived(H.at[yy, (x + 3) % 4, 1 - c], r_hd.at[d * 4 + 1])
        arrived(H.at[yy, (x + 1) % 4, 1 - c], r_hd.at[d * 4 + 2])
        arrived(H.at[yy, (x + 2) % 4, 1 - c], r_hd.at[d * 4 + 3])

    @pl.loop(0, 2)
    def _(t):
        rows = pl.ds(pl.multiple_of(t * 512, 512), 512)
        tokens = H[pl.ds(2 * t, 2)].reshape(512, WIDTH)
        packed = dot(tokens, Wp[...].reshape(6 * PAD, WIDTH), NT).astype(BF16)
        for h in range(2):
            Q[h, rows] = packed[:, (3 * h) * PAD : (3 * h + 1) * PAD]
            K[h, rows] = packed[:, (3 * h + 1) * PAD : (3 * h + 2) * PAD]
            V[h, rows] = packed[:, (3 * h + 2) * PAD : (3 * h + 3) * PAD]

    scale = 1.0 / math.sqrt(HD)
    scale2 = scale * math.log2(math.e)

    wo_near()
    for d in (2, 6):
        wo_second(d)

    @pl.loop(0, 4)
    def _(step):
        row = (y + 3 - step) % 4

        @pl.when(step == 2)
        def _():
            for d in (3, 5, 4):
                wo_second(d)

        @pl.when(step == 3)
        def _():
            for d in (2, 6):
                wo_third(d)

        rows = pl.ds(pl.multiple_of(row * TILE, TILE), TILE)
        for h in range(2):
            scores = dot(Q[h, rows], K[h], NT)
            top = jnp.max(scores, axis=-1, keepdims=True) * scale2
            grown = jnp.exp2(scores * scale2 - top)
            total = jnp.sum(grown, axis=-1, keepdims=True)
            part = (dot(grown.astype(BF16), V[h], NN) * (1.0 / total)).astype(BF16)
            O[h, row] = part.reshape(8, BLOCK, PAD)
            column = jnp.broadcast_to(top + jnp.log2(total), (TILE, PAD))
            LSE[h, :, rows] = jnp.transpose(column)[0:8]

        def give(turn):
            k = (k8 + turn) % 8
            send(O.at[:, row, k], OR.at[:, y, k8], s_oa, r_oa, seq=row * 8 + k)

        for turn in (4, 5, 3, 6, 2, 7, 1):
            give(turn)

        @pl.when(step != 3)
        def _():
            give(0)

    for h in range(2):
        OR[h, y, k8] = O[h, y, k8]

    for d in (3, 5, 4):
        wo_third(d)
    own_wo.wait()

    flat_or = OR.reshape(64, BLOCK, PAD)
    arrived(flat_or.at[pl.ds(0, 62)], r_oa)

    @pl.loop(0, 8)
    def _(turn):
        k = (turn + 2 * (turn % 2)) % 8
        away = shard_offset(k // 2, k % 2)
        kk = (z + away) % 8

        @pl.when(turn != 0)
        def _():
            arrived(half_shard(kk, 1 - c), r_wod.at[(8 - away) % 8])

        heads = jnp.concatenate([OR[h, :, k].reshape(128, PAD) for h in range(2)], axis=-1)
        branch = dot(heads, WO[kk].reshape(2 * PAD, WIDTH), NN)
        RES[...] += branch.reshape(IMAGES, BLOCK, WIDTH)

    RESB[...] = RES[...].reshape(128, WIDTH).astype(BF16)

    @pl.loop(0, 8)
    def _(turn):
        k = ((x + 3 - turn // 2) % 4) * 2 + turn % 2
        kk = (z + shard_offset((k // 2), k % 2)) % 8
        back = dot(RESB[...], WO[kk].reshape(2 * PAD, WIDTH), NT).astype(BF16)
        for h in range(2):
            GS[h, :, k] = back[:, h * PAD : (h + 1) * PAD].reshape(IMAGES, BLOCK, PAD)

        def give(away):
            i = (y + away) % 4
            send(GS.at[:, i, k], GO.at[:, s], s_ga, r_ga, seq=i * 8 + k)

        for away in (2, 1, 3):
            give(away)

        @pl.when(k != k8)
        def _():
            give(0)

    for h in range(2):
        GO[h, s] = GS[h, y, k8]

    flat_go = GO.reshape(64, BLOCK, PAD)
    arrived(flat_go.at[pl.ds(0, 62)], r_ga)

    for h in range(2):
        products = GO[h].reshape(1024, PAD).astype(F32) * O[h].reshape(1024, PAD).astype(F32)
        DOT[h] = jnp.broadcast_to(
            jnp.sum(jnp.transpose(products), axis=0, keepdims=True), (8, 1024)
        )

    GQ[...] = jnp.zeros((2, PAD, 1024), F32)

    def store(block_row, h, kind, value):
        parts = value.astype(BF16).reshape(4, 2, BLOCK, PAD)
        t = h * 3 + kind
        for cc in range(2):
            GP[cc, block_row, :, :, t * PAD : (t + 1) * PAD] = parts[:, cc]

    @pl.loop(0, 4)
    def _(row):
        rows = pl.ds(pl.multiple_of(row * TILE, TILE), TILE)
        for h in range(2):
            queries = Q[h]
            grads = GO[h].reshape(1024, PAD)
            scores = dot(K[h, rows], queries, NT)
            weights = jnp.exp2(scores * scale2 - LSE[h, 0:1])
            grad_values = dot(weights.astype(BF16), grads, NN)
            grad_weights = dot(V[h, rows], grads, NT)
            grad_scores = (weights * (grad_weights - DOT[h, 0:1])).astype(BF16)
            grad_keys = dot(grad_scores, queries, NN) * scale
            grad_query = dot(K[h, rows], grad_scores, TN)

            GQ[h] += grad_query

            store(row, h, 1, grad_keys)
            store(row, h, 2, grad_values)

        for h in range(2):
            lanes = pl.ds((h * 3 + 1) * PAD, 2 * PAD)
            send(
                GP.at[1 - c, row, :, :, lanes], GP2.at[row, :, :, lanes], s_gp, r_gp.at[h, row],
                seq=partner,
            )

    for h in range(2):
        for r in range(4):
            store(r, h, 0, jnp.transpose(GQ[h, :, r * TILE : (r + 1) * TILE]) * scale)
        lanes = pl.ds(h * 3 * PAD, PAD)
        send(GP.at[1 - c, :, :, :, lanes], GP2.at[:, :, :, lanes], s_gp, r_gp.at[h, 4], seq=partner)

    arrived(W2, r_wd)
    for h in range(2):
        for r in range(4):
            arrived(GP2.at[r, :, :, pl.ds((h * 3 + 1) * PAD, 2 * PAD)], r_gp.at[h, r])
        arrived(GP2.at[:, :, :, pl.ds(h * 3 * PAD, PAD)], r_gp.at[h, 4])

    xr, xl, xo = (x + 1) % 4, (x + 3) % 4, (x + 2) % 4

    @pl.loop(0, NSTEPS)
    def _(n):
        lanes = pl.ds(pl.multiple_of(n * NB, NB), NB)
        mine = GP[c].reshape(512, 6 * PAD)
        other = GP2[...].reshape(512, 6 * PAD)
        part = dot(mine, Wp[:, :, lanes].reshape(6 * PAD, NB), NN)
        part = part + dot(other, W2[:, :, lanes].reshape(6 * PAD, NB), NN)
        PF[n] = part.reshape(4, 4, BLOCK, NB)
        PB[n, 0] = PF[n, :, xo, 0:16].astype(BF16)
        PB[n, 1] = PF[n, :, xo, 16:32].astype(BF16)
        send(PB.at[n, 0], R1L.at[n], s_r1, r_r1l.at[n], seq=right)
        send(PB.at[n, 1], R1R.at[n], s_r1, r_r1r.at[n], seq=left)

    @pl.loop(0, NSTEPS)
    def _(n):
        arrived(R1L.at[n], r_r1l.at[n])
        S2R[n, :, 0:16] = (PF[n, :, xr, 0:16] + R1L[n].astype(F32)).astype(BF16)
        S2R[n, :, 16:32] = PF[n, :, xr, 16:32].astype(BF16)
        send(S2R.at[n], R2L.at[n], s_r2, r_r2l.at[n], seq=right)
        arrived(R1R.at[n], r_r1r.at[n])
        S2L[n, :, 16:32] = (PF[n, :, xl, 16:32] + R1R[n].astype(F32)).astype(BF16)
        S2L[n, :, 0:16] = PF[n, :, xl, 0:16].astype(BF16)
        send(S2L.at[n], R2R.at[n], s_r2, r_r2r.at[n], seq=left)

    @pl.loop(0, NSTEPS)
    def _(n):
        arrived(R2L.at[n], r_r2l.at[n])
        arrived(R2R.at[n], r_r2r.at[n])
        total = PF[n, :, x] + R2L[n].astype(F32) + R2R[n].astype(F32)
        YS[n] = total.astype(BF16)
        for d in (2, 1, 3):
            send(
                YS.at[n, (y + d) % 4], YR.at[y, n], s_ry, r_ry.at[d - 1, n],
                seq=at((y + d) % 4, x, c),
            )

    for n in range(NSTEPS):
        YR[y, n] = YS[n, y]

    @pl.loop(0, NSTEPS)
    def _(n):
        for d in range(1, 4):
            arrived(YR.at[(y + d) % 4, n], r_ry.at[3 - d, n])

    lane = lax.broadcasted_iota(jnp.int32, (8, PAD), 1)
    line = lax.broadcasted_iota(jnp.int32, (8, PAD), 0)

    def total_of(value):
        return jnp.sum(jnp.sum(value, axis=0, keepdims=True), axis=1, keepdims=True)

    sums = jnp.zeros((8, PAD), F32)
    for i in range(IMAGES):
        back = jnp.concatenate([YR[i, n] for n in range(NSTEPS)], axis=-1)
        scaled = back.astype(F32) * gain[...].reshape(1, WIDTH)
        unit = normed[i]
        first = jnp.mean(scaled, axis=-1, keepdims=True)
        second = jnp.mean(scaled * unit, axis=-1, keepdims=True)
        gradient = RES[i] + (scaled - first - unit * second) * inv[i][:, 0:1]
        RES[i] = gradient
        pltpu.make_async_copy(RES.at[i], grad_out.at[i], l_out.at[i]).start()
        current = pert[i]
        for j, value in enumerate((gradient * gradient, current * gradient, current * current)):
            sums = jnp.where((line == i) & (lane == j), total_of(value), sums)
    SC[...] = sums
    SCR[s] = sums

    for d in (18, 20, 22, 16, 17, 19, 21, 23, *range(8, 16), *range(24, 32), *range(1, 8)):
        send(SC, SCR.at[s], s_sc, r_sc, seq=(s + d) % SEQ)

    arrived(SCR.at[pl.ds(0, SEQ - 1)], r_sc)
    sums = jnp.sum(SCR[...], axis=0)
    column = lax.broadcasted_iota(jnp.int32, (8, 1), 0)
    step_of, radius_of = jnp.ones((8, 1), F32), jnp.ones((8, 1), F32)
    for i in range(IMAGES):
        step_of = jnp.where(column == i, stp[z * IMAGES + i], step_of)
        radius_of = jnp.where(column == i, rad[z * IMAGES + i], radius_of)
    grad_square, cross, own = sums[:, 0:1], sums[:, 1:2], sums[:, 2:3]
    factor = step_of / jnp.sqrt(grad_square + norm_epsilon)
    stepped_square = own + 2.0 * factor * cross + factor * factor * grad_square
    shrink = jnp.minimum(1.0, radius_of / jnp.sqrt(stepped_square + norm_epsilon))
    shrink_row, factor_row = jnp.zeros((1, PAD), F32), jnp.zeros((1, PAD), F32)
    for i in range(IMAGES):
        shrink_row = jnp.where(lane[0:1] == i, shrink[i : i + 1], shrink_row)
        factor_row = jnp.where(lane[0:1] == i, (factor * shrink)[i : i + 1], factor_row)
    shrink_out[...] = shrink_row.reshape(PAD)
    factor_out[...] = factor_row.reshape(PAD)
    for i in range(IMAGES):
        pltpu.make_async_copy(RES.at[i], grad_out.at[i], l_out.at[i]).wait()

    @pl.when(offset != 0)
    def _():
        for q in range(CHUNKS):
            arrived(source(q), s_wz)

    @pl.when(offset == 4)
    def _():
        arrived(RB, s_rb)

    for q in range(CHUNKS):
        for _ in range(3):
            arrived(source(q), s_wy)
    arrived(HS.at[pl.ds(0, 3)], s_hy)
    arrived(H.at[0, :, :].reshape(8, BLOCK, WIDTH), s_hx)
    arrived(H.at[0, pl.ds(0, 2)].reshape(4, BLOCK, WIDTH), s_hx)
    arrived(H.at[pl.ds(0, 2)].reshape(16, BLOCK, WIDTH), s_hd)
    arrived(Wp, s_wd)
    for d in range(1, PLANES):
        arrived(piece(wo_own, y, c), s_wo)
        if d in (1, 7):
            for _ in range(3):
                arrived(piece(wo_own, y, c), s_wo)
        else:
            for _ in range(3):
                arrived(piece(wo_own, y, c), s_woy)
        arrived(half_shard(z, c), s_wod)
    arrived(flat_or.at[pl.ds(0, 62)], s_oa)
    arrived(flat_go.at[pl.ds(0, 62)], s_ga)
    arrived(GP2, s_gp)
    arrived(PB, s_r1)
    arrived(S2R, s_r2)
    arrived(S2L, s_r2)
    for _ in range(3):
        arrived(YR.at[pl.ds(0, 1)], s_ry)
    arrived(SCR.at[pl.ds(0, SEQ - 1)], s_sc)


def on_device(patch_embed, perturbation, target, ln_gain, ln_bias, w_qkv, w_out, radius, step_size):
    vmem = pl.BlockSpec(memory_space=pltpu.VMEM)
    anywhere = pl.BlockSpec(memory_space=pl.ANY)
    dma = pltpu.SemaphoreType.DMA
    V = pltpu.VMEM
    scratch = [
        V(patch_embed.shape, BF16),
        V(perturbation.shape, F32),
        V(target.shape, BF16),
        V(ln_gain.shape, F32),
        V(ln_bias.shape, F32),
        pltpu.SMEM(radius.shape, F32),
        pltpu.SMEM(step_size.shape, F32),
        V((4, 4, 2, BLOCK, WIDTH), BF16),
        V((4, CHUNK, WIDTH // 2), BF16),
        V((6, PAD, WIDTH), BF16),
        V((6, PAD, WIDTH), BF16),
        V((PLANES, 2, PAD, WIDTH), BF16),
        V((IMAGES, BLOCK, WIDTH), F32),
        V((IMAGES, BLOCK, PAD), F32),
        V((IMAGES, BLOCK, WIDTH), BF16),
        V((2, 1024, PAD), BF16),
        V((2, 1024, PAD), BF16),
        V((2, 1024, PAD), BF16),
        V((2, 4, 8, BLOCK, PAD), BF16),
        V((2, 4, 8, BLOCK, PAD), BF16),
        V((2, 8, 1024), F32),
        V((2, 8, 1024), F32),
        V((2, 4, 8, BLOCK, PAD), BF16),
        V((2, 32, BLOCK, PAD), BF16),
        V((2, PAD, 1024), F32),
        V((2, 4, 4, BLOCK, 6 * PAD), BF16),
        V((4, 4, BLOCK, 6 * PAD), BF16),
        V((IMAGES, BLOCK, WIDTH), F32),
        V((IMAGES * BLOCK, WIDTH), BF16),
        V((NSTEPS, 4, 4, BLOCK, NB), F32),
        V((NSTEPS, 2, 4, 16, NB), BF16),
        V((NSTEPS, 4, 16, NB), BF16),
        V((NSTEPS, 4, 16, NB), BF16),
        V((NSTEPS, 4, BLOCK, NB), BF16),
        V((NSTEPS, 4, BLOCK, NB), BF16),
        V((NSTEPS, 4, BLOCK, NB), BF16),
        V((NSTEPS, 4, BLOCK, NB), BF16),
        V((NSTEPS, 4, BLOCK, NB), BF16),
        V((4, NSTEPS, BLOCK, NB), BF16),
        V((8, PAD), F32),
        V((SEQ, 8, PAD), F32),
        dma((7,)), dma((IMAGES,)), dma, dma((4,)),
        dma, dma((CHUNKS,)), dma, dma((CHUNKS,)), dma((CHUNKS,)), dma((CHUNKS,)),
        dma, dma((3,)), dma, dma((4,)), dma((4,)), dma((4,)), dma((4,)),
        dma, dma((16,)),
        dma, dma((8,)), dma((2, 3)), dma, dma((8,)), dma((8,)), dma((8,)), dma, dma((8,)), dma,
        dma, dma,
        dma, dma, dma, dma,
        dma, dma((2, 5)),
        dma, dma((NSTEPS,)), dma((NSTEPS,)),
        dma, dma((NSTEPS,)), dma((NSTEPS,)),
        dma, dma((3, NSTEPS)),
        dma, dma,
    ]
    gradient, shrink, factor = pl.pallas_call(
        kernel,
        out_shape=(
            jax.ShapeDtypeStruct(perturbation.shape, F32),
            jax.ShapeDtypeStruct((PAD,), F32),
            jax.ShapeDtypeStruct((PAD,), F32),
        ),
        in_specs=[anywhere] * 9,
        out_specs=(anywhere, vmem, vmem),
        scratch_shapes=scratch,
        compiler_params=pltpu.CompilerParams(
            collective_id=0, has_side_effects=True, vmem_limit_bytes=62 * 1024 * 1024
        ),
    )(
        patch_embed,
        perturbation,
        target,
        ln_gain,
        ln_bias,
        w_qkv.reshape(12, CHUNK, WIDTH),
        w_out,
        radius,
        step_size,
    )
    return perturbation * shrink[:IMAGES, None, None] + factor[:IMAGES, None, None] * gradient


def solution(mesh):
    placed = (
        P("head", "seq", None),
        P("head", "seq", None),
        P("head", "seq", None),
        P(),
        P(),
        P("head", None, None),
        P("head", None, None),
        P(),
        P(),
    )
    return jax.shard_map(
        on_device, mesh=mesh, in_specs=placed, out_specs=P("head", "seq", None), check_vma=False
    )
```

```python
import functools
import math

import jax
import jax.numpy as jnp
from jax import lax
from jax.experimental import pallas as pl
from jax.experimental.pallas import tpu as pltpu
from jax.sharding import PartitionSpec as P

norm_epsilon = 1e-06
layer_epsilon = 1e-06

F32 = jnp.float32
BF16 = jnp.bfloat16
NT = (((1,), (1,)), ((), ()))
NN = (((1,), (0,)), ((), ()))
TN = (((0,), (0,)), ((), ()))

IMAGES = 4
ROWS = 4
COLS = 4
PLANES = 8
SEQ = 32
BLOCK = 32
WIDTH = 1280
HD = 80
PACKED = 40
PAD = 128
CHUNK = 40
NB = 256
NSTEPS = WIDTH // NB
CHUNKS = 6
TILE = 256


def dot(a, b, dims):
    return lax.dot_general(a, b, dims, preferred_element_type=F32)


def lane_of(value):
    return lax.broadcasted_iota(jnp.int32, value.shape, value.ndim - 1)


def pack_rest(rest):
    groups = rest.reshape(-1, 4, 8, PAD)
    packed = groups[:, 0].reshape(-1, PAD)
    lane = lane_of(packed)
    for g in range(1, 4):
        turned = pltpu.roll(groups[:, g].reshape(-1, PAD), 32 * g, 1)
        packed = jnp.where(lane >= 32 * g, turned, packed)
    return packed.reshape(-1, 8, PAD)


def unpack_rest(packed, lane):
    flat = packed.reshape(-1, PAD)
    groups = [
        pltpu.roll(flat, (PAD + lane - 32 * g) % PAD, 1).reshape(-1, 1, 8, PAD) for g in range(4)
    ]
    return jnp.concatenate(groups, axis=1).reshape(-1, PAD)


def shard_offset(x, c):
    other = 8 - x - 4 * (1 - (x + 3) // 4)
    return (1 - c) * x + c * other


def kernel(
    pe_in, pert_in, tgt_in, gain_in, bias_in, w_own, wo_own, rad_in, stp_in, grad_out, shrink_out, factor_out,
    pe, pert, tgt, gain, bias, rad, stp,
    H, RB, Wp, W2, WO, normed, inv, HS, Q, K, V, O, OS, OR, LSE, DOT, GS, GO, GH, GQ, GP, GP2,
    RES, RESB, PF, PB, R1L, R1R, S2L, S2R, R2L, R2R, YS, YR, SC, SCR, SHRINK, FACTOR,
    l_in, l_out, l_res, s_rb, r_rb, s_wz, r_wz, s_wy, r_wyl, r_wyr, r_wyy, s_hy, r_hy, s_hx, r_hxl, r_hxr, r_hxy, r_hxz,
    s_hd, r_hd, s_wo, r_wo, r_wof, s_woy, r_wol, r_wor, r_woz, s_wod, r_wod, l_wo, s_wd, r_wd, s_oa, r_oa, s_ga, r_ga,
    s_gp, r_gp, s_r1, r_r1l, r_r1r, s_r2, r_r2l, r_r2r, s_ry, r_ry, s_sc, r_sc,
):
    s = lax.axis_index("seq")
    z = lax.axis_index("head")
    y = s // 8
    x = (s // 2) % 4
    c = s % 2
    k8 = s % 8

    def at(yy, xx, cc):
        return (yy * 4 + xx) * 2 + cc

    right = at(y, (x + 1) % 4, c)
    left = at(y, (x + 3) % 4, c)
    down = at((y + 1) % 4, x, c)
    up = at((y + 3) % 4, x, c)
    partner = at(y, x, 1 - c)

    def send(src, dst, ssem, rsem, **where):
        copy = pltpu.make_async_remote_copy(
            src_ref=src, dst_ref=dst, send_sem=ssem, recv_sem=rsem,
            device_id=where, device_id_type=pl.DeviceIdType.MESH,
        )
        copy.start()

    def arrived(ref, sem):
        pltpu.make_async_copy(ref, ref, sem).wait()

    loads = [
        pltpu.make_async_copy(src, dst, l_in.at[i])
        for i, (src, dst) in enumerate(
            ((pe_in, pe), (pert_in, pert), (gain_in, gain), (bias_in, bias), (tgt_in, tgt),
             (rad_in, rad), (stp_in, stp))
        )
    ]
    for load in loads:
        load.start()

    barrier = pltpu.get_barrier_semaphore()

    for d in range(1, SEQ):
        pl.semaphore_signal(
            barrier, inc=1, device_id={"seq": (s + d) % SEQ}, device_id_type=pl.DeviceIdType.MESH
        )
    for d in range(1, PLANES):
        pl.semaphore_signal(
            barrier, inc=1, device_id={"head": (z + d) % PLANES},
            device_id_type=pl.DeviceIdType.MESH,
        )

    own_wo = pltpu.make_async_copy(wo_own, WO.at[z, pl.ds(0, 2 * HD)], l_wo)
    own_wo.start()

    def normalize(image):
        mixed = pe[image].astype(F32) + pert[image]
        rounded = mixed.astype(BF16).astype(F32)
        center = rounded - jnp.mean(rounded, axis=-1, keepdims=True)
        variance = jnp.mean(center * center, axis=-1, keepdims=True)
        inverse = lax.rsqrt(variance + layer_epsilon)
        return mixed, center * inverse, inverse

    def layer_norm(image):
        _, unit, _ = normalize(image)
        return (unit * gain[...].reshape(1, WIDTH) + bias[...].reshape(1, WIDTH)).astype(BF16)

    for load in loads[:4]:
        load.wait()

    @pl.loop(1, ROWS)
    def _(d):
        image = (y + d) % 4
        HS[image] = layer_norm(image)

    H[y, x, c] = layer_norm(y)

    pl.semaphore_wait(barrier, SEQ - 1 + PLANES - 1)

    offset = shard_offset(x, c)
    target = (z + 8 - offset) % 8

    half_width = WIDTH // 2

    def ways(plane):
        odd = plane % 2
        place = odd * y + (1 - odd) * x
        return place, odd * down + (1 - odd) * right, odd * up + (1 - odd) * left

    def piece(ref, place, cc):
        rows = pl.ds(pl.multiple_of(CHUNK * place, 8), CHUNK)
        lanes = pl.ds(pl.multiple_of(cc * half_width, PAD), half_width)
        return ref.at[rows, lanes]

    def half_shard(plane, cc):
        lanes = pl.ds(pl.multiple_of(cc * half_width, PAD), half_width)
        return WO.at[plane, pl.ds(0, 2 * HD), lanes]

    place, _, _ = ways(z)
    for d in (1, 7):
        send(piece(wo_own, place, c), piece(WO.at[z], place, c), s_wo, r_wo.at[d], head=(z + d) % 8)

    def chunk(yy, q):
        u = 3 * yy + q % 3
        rows = pl.ds(pl.multiple_of(CHUNK * (u % 2), 8), CHUNK)
        return Wp.at[u // 2, rows, pl.ds((q // 3) * half_width, half_width)]

    def source(q):
        return w_own.at[3 * y + q % 3, :, pl.ds((q // 3) * half_width, half_width)]

    between = {0: (0, 2), 1: (1, 6), 3: (2, 2), 4: (3, 6)}

    for q in range(CHUNKS):
        @pl.when(offset == 0)
        def _():
            pltpu.make_async_copy(source(q), chunk(y, q), r_wz.at[q]).start()

        if q in between:
            slot, hop = between[q]

            @pl.when(offset == 4)
            def _():
                send(source(q), RB.at[slot], s_wz, r_rb.at[slot], head=(z + hop) % 8)

            @pl.when((offset != 0) & (offset != 4))
            def _():
                send(source(q), chunk(y, q), s_wz, r_wz.at[q], head=target)
        else:
            @pl.when(offset != 0)
            def _():
                send(source(q), chunk(y, q), s_wz, r_wz.at[q], head=target)

    def pass_on(q):
        slot, hop = between[q]

        @pl.when(offset == 4)
        def _():
            arrived(RB.at[slot], r_rb.at[slot])
            send(RB.at[slot], chunk(y, q), s_rb, r_wz.at[q], head=(z + hop) % 8)

    @pl.loop(1, ROWS)
    def _(d):
        image = (y + d) % 4
        send(HS.at[image], H.at[y, x, c], s_hy, r_hy.at[d - 1], seq=at(image, x, c))

    def spread(d):
        yy = (y + d) % 4
        block = H.at[yy, x, c]
        send(block, block, s_hx, r_hxl.at[d], seq=right)
        send(block, block, s_hx, r_hxr.at[d], seq=left)
        send(block, block, s_hd, r_hd.at[d * 4], seq=partner)

    def relay(d):
        yy = (y + d) % 4
        from_left = H.at[yy, (x + 3) % 4, c]
        arrived(from_left, r_hxl.at[d])
        upper = H.at[yy, (x + 3) % 4, c, pl.ds(0, 16)]
        send(upper, upper, s_hx, r_hxy.at[d], seq=right)
        send(from_left, from_left, s_hd, r_hd.at[d * 4 + 1], seq=partner)
        from_right = H.at[yy, (x + 1) % 4, c]
        arrived(from_right, r_hxr.at[d])
        lower = H.at[yy, (x + 1) % 4, c, pl.ds(16, 16)]
        send(lower, lower, s_hx, r_hxz.at[d], seq=left)
        send(from_right, from_right, s_hd, r_hd.at[d * 4 + 2], seq=partner)

    def from_row(d):
        arrived(H.at[(y + d) % 4, x, c], r_hy.at[3 - d])
        spread(d)

    def round_column(j):
        arrived(chunk(y, j), r_wz.at[j])
        send(chunk(y, j), chunk(y, j), s_wy, r_wyl.at[j], seq=down)
        send(chunk(y, j), chunk(y, j), s_wy, r_wyr.at[j], seq=up)

    def wo_chain(step):
        for d, ahead, there, last in ((step, 1, step + 1, 4), (8 - step, 7, 7 - step, 5)):
            if step == 4 and ahead == 7:
                continue
            plane = (z + 8 - d) % 8
            place, _, _ = ways(plane)
            got = piece(WO.at[plane], place, c)
            arrived(got, r_wo.at[d])
            if d != last:
                send(got, got, s_wo, r_wo.at[there], head=(z + ahead) % 8)

    def wo_give():
        place, _, _ = ways(z)
        for i, d in enumerate((1, 7)):
            for part in range(3):
                spot = (place + 1 + part) % 4
                send(
                    piece(wo_own, spot, c), piece(WO.at[z], spot, c), s_wo, r_wof.at[i, part],
                    head=(z + d) % 8,
                )

    def wo_near():
        for i, d in enumerate((1, 7)):
            plane = (z + 8 - d) % 8
            place, _, _ = ways(plane)
            for part in range(3):
                arrived(piece(WO.at[plane], (place + 1 + part) % 4, c), r_wof.at[i, part])
            send(half_shard(plane, c), half_shard(plane, c), s_wod, r_wod.at[d], seq=partner)

    def wo_first(d):
        plane = (z + 8 - d) % 8
        place, after, before = ways(plane)
        got = piece(WO.at[plane], place, c)
        send(got, got, s_woy, r_wol.at[d], seq=after)
        send(got, got, s_woy, r_wor.at[d], seq=before)
        send(got, got, s_wod, r_wod.at[d], seq=partner)

    def wo_second(d):
        plane = (z + 8 - d) % 8
        place, after, before = ways(plane)
        shard = WO.at[plane]
        lower, upper = piece(shard, (place + 3) % 4, c), piece(shard, (place + 1) % 4, c)
        arrived(lower, r_wol.at[d])
        arrived(upper, r_wor.at[d])
        send(lower, lower, s_wod, r_wod.at[d], seq=partner)
        send(upper, upper, s_wod, r_wod.at[d], seq=partner)
        turn = (plane // 2) % 2

        @pl.when(turn == 0)
        def _():
            send(lower, lower, s_woy, r_woz.at[d], seq=after)

        @pl.when(turn == 1)
        def _():
            send(upper, upper, s_woy, r_woz.at[d], seq=before)

    def wo_third(d):
        plane = (z + 8 - d) % 8
        place, _, _ = ways(plane)
        got = piece(WO.at[plane], (place + 2) % 4, c)
        arrived(got, r_woz.at[d])
        send(got, got, s_wod, r_wod.at[d], seq=partner)

    yu, yd, yo = (y + 3) % 4, (y + 1) % 4, (y + 2) % 4

    def relay_column(q):
        arrived(chunk(yu, q), r_wyl.at[q])
        arrived(chunk(yd, q), r_wyr.at[q])
        if q % 2 == 0:
            send(chunk(yu, q), chunk(yu, q), s_wy, r_wyy.at[q], seq=down)
        else:
            send(chunk(yd, q), chunk(yd, q), s_wy, r_wyy.at[q], seq=up)

    def far_column(d):
        yy, xx = (y + d) % 4, (x + 2) % 4
        arrived(H.at[yy, xx, c, pl.ds(0, 16)], r_hxy.at[d])
        arrived(H.at[yy, xx, c, pl.ds(16, 16)], r_hxz.at[d])
        send(H.at[yy, xx, c], H.at[yy, xx, c], s_hd, r_hd.at[d * 4 + 3], seq=partner)

    spread(0)

    @pl.loop(0, 6)
    def _(t):
        Wp[t, HD:PAD, :] = jnp.zeros((PAD - HD, WIDTH), BF16)

    @pl.loop(0, PLANES)
    def _(t):
        WO[t, 2 * HD : 2 * PAD, :] = jnp.zeros((2 * (PAD - HD), WIDTH), BF16)

    for load in loads[4:]:
        load.wait()

    @pl.loop(0, IMAGES)
    def _(image):
        mixed, unit, inverse = normalize(image)
        normed[image] = unit
        inv[image] = jnp.broadcast_to(inverse, (BLOCK, PAD))
        RES[image] = mixed - tgt[image].astype(F32)

    from_row(1)
    relay(0)
    wo_chain(1)
    from_row(3)
    pass_on(0)
    pass_on(1)
    from_row(2)
    round_column(0)
    round_column(1)
    pass_on(3)
    pass_on(4)
    relay(1)
    round_column(2)
    relay_column(0)
    relay(3)
    wo_chain(2)
    relay_column(1)
    relay(2)
    round_column(3)
    relay_column(2)
    round_column(4)
    far_column(0)
    round_column(5)
    wo_give()
    relay_column(3)
    wo_chain(3)
    wo_first(2)
    wo_first(6)
    far_column(1)
    relay_column(4)
    far_column(3)
    relay_column(5)
    far_column(2)

    for q in range(CHUNKS):
        arrived(chunk(yo, q), r_wyy.at[q])

    send(Wp, W2, s_wd, r_wd, seq=partner)
    wo_chain(4)
    for d in (3, 5, 4):
        wo_first(d)

    @pl.loop(0, ROWS)
    def _(d):
        yy = (y + d) % 4
        arrived(H.at[yy, x, 1 - c], r_hd.at[d * 4])
        arrived(H.at[yy, (x + 3) % 4, 1 - c], r_hd.at[d * 4 + 1])
        arrived(H.at[yy, (x + 1) % 4, 1 - c], r_hd.at[d * 4 + 2])
        arrived(H.at[yy, (x + 2) % 4, 1 - c], r_hd.at[d * 4 + 3])

    @pl.loop(0, 2)
    def _(t):
        rows = pl.ds(pl.multiple_of(t * 512, 512), 512)
        tokens = H[pl.ds(2 * t, 2)].reshape(512, WIDTH)
        packed = dot(tokens, Wp[...].reshape(6 * PAD, WIDTH), NT).astype(BF16)
        for h in range(2):
            Q[h, rows] = packed[:, (3 * h) * PAD : (3 * h + 1) * PAD]
            K[h, rows] = packed[:, (3 * h + 1) * PAD : (3 * h + 2) * PAD]
            V[h, rows] = packed[:, (3 * h + 2) * PAD : (3 * h + 3) * PAD]

    scale = 1.0 / math.sqrt(HD)
    scale2 = scale * math.log2(math.e)

    wo_near()
    for d in (2, 6):
        wo_second(d)

    @pl.loop(0, 4)
    def _(step):
        row = (y + 3 - step) % 4

        @pl.when(step == 2)
        def _():
            for d in (3, 5, 4):
                wo_second(d)

        @pl.when(step == 3)
        def _():
            for d in (2, 6):
                wo_third(d)

        rows = pl.ds(pl.multiple_of(row * TILE, TILE), TILE)
        parts = []
        for h in range(2):
            scores = dot(Q[h, rows], K[h], NT)
            top = jnp.max(scores, axis=-1, keepdims=True) * scale2
            grown = jnp.exp2(scores * scale2 - top)
            total = jnp.sum(grown, axis=-1, keepdims=True)
            part = dot(grown.astype(BF16), V[h], NN) * (1.0 / total)
            parts.append(part)
            O[h, row] = part.astype(BF16).reshape(8, BLOCK, PAD)
            column = jnp.broadcast_to(top + jnp.log2(total), (TILE, PAD))
            LSE[h, :, rows] = jnp.transpose(column)[0:8]

        turned = pltpu.roll(parts[1], HD, 1)
        whole = jnp.where(lane_of(turned) < HD, parts[0], turned)
        OS[row, :, 0:BLOCK] = whole.astype(BF16).reshape(8, BLOCK, PAD)
        OS[row, :, BLOCK:PACKED] = pack_rest(turned).astype(BF16)

        def give(turn):
            k = (k8 + turn) % 8
            send(OS.at[row, k], OR.at[s], s_oa, r_oa, seq=row * 8 + k)

        for turn in (4, 5, 3, 6, 2, 7, 1):
            give(turn)

        @pl.when(step != 3)
        def _():
            give(0)

    OR[s] = OS[y, k8]

    for d in (3, 5, 4):
        wo_third(d)
    own_wo.wait()

    arrived(OR.at[pl.ds(0, SEQ - 1)], r_oa)

    @pl.loop(0, 8)
    def _(turn):
        k = (turn + 2 * (turn % 2)) % 8
        away = shard_offset(k // 2, k % 2)
        kk = (z + away) % 8

        @pl.when(turn != 0)
        def _():
            arrived(half_shard(kk, 1 - c), r_wod.at[(8 - away) % 8])

        rest = jnp.concatenate([OR[i * 8 + k, BLOCK:PACKED] for i in range(IMAGES)], axis=0)
        rest = unpack_rest(rest.astype(F32), 0)
        rest = jnp.where(lane_of(rest) < 32, rest, 0.0).astype(BF16)
        whole = jnp.concatenate([OR[i * 8 + k, 0:BLOCK] for i in range(IMAGES)], axis=0)
        heads = jnp.concatenate([whole, rest], axis=-1)
        branch = dot(heads, WO[kk], NN)
        RES[...] += branch.reshape(IMAGES, BLOCK, WIDTH)

    RESB[...] = RES[...].reshape(128, WIDTH).astype(BF16)

    @pl.loop(0, 8)
    def _(turn):
        k = ((x + 3 - turn // 2) % 4) * 2 + turn % 2
        kk = (z + shard_offset((k // 2), k % 2)) % 8
        back = dot(RESB[...], WO[kk], NT)
        GS[:, k, 0:BLOCK] = back[:, 0:PAD].astype(BF16).reshape(IMAGES, BLOCK, PAD)
        GS[:, k, BLOCK:PACKED] = pack_rest(back[:, PAD : 2 * PAD]).astype(BF16)

        def give(away):
            i = (y + away) % 4
            send(GS.at[i, k], GO.at[s], s_ga, r_ga, seq=i * 8 + k)

        for away in (2, 1, 3):
            give(away)

        @pl.when(k != k8)
        def _():
            give(0)

    GO[s] = GS[y, k8]

    arrived(GO.at[pl.ds(0, SEQ - 1)], r_ga)

    @pl.loop(0, 4)
    def _(row):
        blocks = pl.ds(row * 8, 8)
        rows = pl.ds(pl.multiple_of(row * TILE, TILE), TILE)
        whole = GO[blocks, 0:BLOCK].astype(F32).reshape(TILE, PAD)
        rest = unpack_rest(GO[blocks, BLOCK:PACKED].astype(F32), PAD - HD)
        lane = lane_of(whole)
        turned = pltpu.roll(whole, PAD - HD, 1)
        GH[0, rows] = jnp.where(lane < HD, whole, 0.0).astype(BF16)
        GH[1, rows] = jnp.where(
            lane < PAD - HD, turned, jnp.where(lane < HD, rest, 0.0)
        ).astype(BF16)

    for h in range(2):
        products = GH[h].astype(F32) * O[h].reshape(1024, PAD).astype(F32)
        DOT[h] = jnp.broadcast_to(
            jnp.sum(jnp.transpose(products), axis=0, keepdims=True), (8, 1024)
        )

    GQ[...] = jnp.zeros((2, PAD, 1024), F32)

    def store(block_row, h, kind, value):
        parts = value.astype(BF16).reshape(4, 2, BLOCK, PAD)
        t = h * 3 + kind
        for cc in range(2):
            GP[cc, block_row, :, :, t * PAD : (t + 1) * PAD] = parts[:, cc]

    @pl.loop(0, 4)
    def _(row):
        rows = pl.ds(pl.multiple_of(row * TILE, TILE), TILE)
        for h in range(2):
            queries = Q[h]
            grads = GH[h]
            scores = dot(K[h, rows], queries, NT)
            weights = jnp.exp2(scores * scale2 - LSE[h, 0:1])
            grad_values = dot(weights.astype(BF16), grads, NN)
            grad_weights = dot(V[h, rows], grads, NT)
            grad_scores = (weights * (grad_weights - DOT[h, 0:1])).astype(BF16)
            grad_keys = dot(grad_scores, queries, NN) * scale
            grad_query = dot(K[h, rows], grad_scores, TN)

            GQ[h] += grad_query

            store(row, h, 1, grad_keys)
            store(row, h, 2, grad_values)

        for h in range(2):
            lanes = pl.ds((h * 3 + 1) * PAD, 2 * PAD)
            send(
                GP.at[1 - c, row, :, :, lanes], GP2.at[row, :, :, lanes], s_gp, r_gp.at[h, row],
                seq=partner,
            )

    for h in range(2):
        for r in range(4):
            store(r, h, 0, jnp.transpose(GQ[h, :, r * TILE : (r + 1) * TILE]) * scale)
        lanes = pl.ds(h * 3 * PAD, PAD)
        send(GP.at[1 - c, :, :, :, lanes], GP2.at[:, :, :, lanes], s_gp, r_gp.at[h, 4], seq=partner)

    arrived(W2, r_wd)
    for h in range(2):
        for r in range(4):
            arrived(GP2.at[r, :, :, pl.ds((h * 3 + 1) * PAD, 2 * PAD)], r_gp.at[h, r])
        arrived(GP2.at[:, :, :, pl.ds(h * 3 * PAD, PAD)], r_gp.at[h, 4])

    xr, xl, xo = (x + 1) % 4, (x + 3) % 4, (x + 2) % 4

    @pl.loop(0, NSTEPS)
    def _(n):
        lanes = pl.ds(pl.multiple_of(n * NB, NB), NB)
        mine = GP[c].reshape(512, 6 * PAD)
        other = GP2[...].reshape(512, 6 * PAD)
        part = dot(mine, Wp[:, :, lanes].reshape(6 * PAD, NB), NN)
        part = part + dot(other, W2[:, :, lanes].reshape(6 * PAD, NB), NN)
        PF[n] = part.reshape(4, 4, BLOCK, NB)
        PB[n, 0] = PF[n, :, xo, 0:16].astype(BF16)
        PB[n, 1] = PF[n, :, xo, 16:32].astype(BF16)
        send(PB.at[n, 0], R1L.at[n], s_r1, r_r1l.at[n], seq=right)
        send(PB.at[n, 1], R1R.at[n], s_r1, r_r1r.at[n], seq=left)

    @pl.loop(0, NSTEPS)
    def _(n):
        arrived(R1L.at[n], r_r1l.at[n])
        S2R[n, :, 0:16] = (PF[n, :, xr, 0:16] + R1L[n].astype(F32)).astype(BF16)
        S2R[n, :, 16:32] = PF[n, :, xr, 16:32].astype(BF16)
        send(S2R.at[n], R2L.at[n], s_r2, r_r2l.at[n], seq=right)
        arrived(R1R.at[n], r_r1r.at[n])
        S2L[n, :, 16:32] = (PF[n, :, xl, 16:32] + R1R[n].astype(F32)).astype(BF16)
        S2L[n, :, 0:16] = PF[n, :, xl, 0:16].astype(BF16)
        send(S2L.at[n], R2R.at[n], s_r2, r_r2r.at[n], seq=left)

    @pl.loop(0, NSTEPS)
    def _(n):
        arrived(R2L.at[n], r_r2l.at[n])
        arrived(R2R.at[n], r_r2r.at[n])
        total = PF[n, :, x] + R2L[n].astype(F32) + R2R[n].astype(F32)
        YS[n] = total.astype(BF16)
        for d in (2, 1, 3):
            send(
                YS.at[n, (y + d) % 4], YR.at[y, n], s_ry, r_ry.at[d - 1, n],
                seq=at((y + d) % 4, x, c),
            )

    for n in range(NSTEPS):
        YR[y, n] = YS[n, y]

    @pl.loop(0, NSTEPS)
    def _(n):
        for d in range(1, 4):
            arrived(YR.at[(y + d) % 4, n], r_ry.at[3 - d, n])

    lane = lax.broadcasted_iota(jnp.int32, (8, PAD), 1)
    line = lax.broadcasted_iota(jnp.int32, (8, PAD), 0)

    def total_of(value):
        return jnp.sum(jnp.sum(value, axis=0, keepdims=True), axis=1, keepdims=True)

    sums = jnp.zeros((8, PAD), F32)
    for i in range(IMAGES):
        back = jnp.concatenate([YR[i, n] for n in range(NSTEPS)], axis=-1)
        scaled = back.astype(F32) * gain[...].reshape(1, WIDTH)
        unit = normed[i]
        first = jnp.mean(scaled, axis=-1, keepdims=True)
        second = jnp.mean(scaled * unit, axis=-1, keepdims=True)
        gradient = RES[i] + (scaled - first - unit * second) * inv[i][:, 0:1]
        RES[i] = gradient
        pltpu.make_async_copy(RES.at[i], grad_out.at[i], l_out.at[i]).start()
        current = pert[i]
        for j, value in enumerate((gradient * gradient, current * gradient, current * current)):
            sums = jnp.where((line == i) & (lane == j), total_of(value), sums)
    SC[...] = sums
    SCR[s] = sums

    for d in (18, 20, 22, 16, 17, 19, 21, 23, *range(8, 16), *range(24, 32), *range(1, 8)):
        send(SC, SCR.at[s], s_sc, r_sc, seq=(s + d) % SEQ)

    arrived(SCR.at[pl.ds(0, SEQ - 1)], r_sc)
    sums = jnp.sum(SCR[...], axis=0)
    column = lax.broadcasted_iota(jnp.int32, (8, 1), 0)
    step_of, radius_of = jnp.ones((8, 1), F32), jnp.ones((8, 1), F32)
    for i in range(IMAGES):
        step_of = jnp.where(column == i, stp[z * IMAGES + i], step_of)
        radius_of = jnp.where(column == i, rad[z * IMAGES + i], radius_of)
    grad_square, cross, own = sums[:, 0:1], sums[:, 1:2], sums[:, 2:3]
    factor = step_of / jnp.sqrt(grad_square + norm_epsilon)
    stepped_square = own + 2.0 * factor * cross + factor * factor * grad_square
    shrink = jnp.minimum(1.0, radius_of / jnp.sqrt(stepped_square + norm_epsilon))
    shrink_row, factor_row = jnp.zeros((1, PAD), F32), jnp.zeros((1, PAD), F32)
    for i in range(IMAGES):
        shrink_row = jnp.where(lane[0:1] == i, shrink[i : i + 1], shrink_row)
        factor_row = jnp.where(lane[0:1] == i, (factor * shrink)[i : i + 1], factor_row)
    SHRINK[...] = shrink_row.reshape(PAD)
    FACTOR[...] = factor_row.reshape(PAD)
    results = [
        pltpu.make_async_copy(SHRINK, shrink_out, l_res.at[0]),
        pltpu.make_async_copy(FACTOR, factor_out, l_res.at[1]),
    ]
    for result in results:
        result.start()
    for i in range(IMAGES):
        pltpu.make_async_copy(RES.at[i], grad_out.at[i], l_out.at[i]).wait()

    @pl.when(offset != 0)
    def _():
        for q in range(CHUNKS):
            arrived(source(q), s_wz)

    @pl.when(offset == 4)
    def _():
        arrived(RB, s_rb)

    for q in range(CHUNKS):
        for _ in range(3):
            arrived(source(q), s_wy)
    arrived(HS.at[pl.ds(0, 3)], s_hy)
    arrived(H.at[0, :, :].reshape(8, BLOCK, WIDTH), s_hx)
    arrived(H.at[0, pl.ds(0, 2)].reshape(4, BLOCK, WIDTH), s_hx)
    arrived(H.at[pl.ds(0, 2)].reshape(16, BLOCK, WIDTH), s_hd)
    arrived(Wp, s_wd)
    for d in range(1, PLANES):
        arrived(piece(wo_own, y, c), s_wo)
        if d in (1, 7):
            for _ in range(3):
                arrived(piece(wo_own, y, c), s_wo)
        else:
            for _ in range(3):
                arrived(piece(wo_own, y, c), s_woy)
        arrived(half_shard(z, c), s_wod)
    arrived(OR.at[pl.ds(0, SEQ - 1)], s_oa)
    arrived(GO.at[pl.ds(0, SEQ - 1)], s_ga)
    arrived(GP2, s_gp)
    arrived(PB, s_r1)
    arrived(S2R, s_r2)
    arrived(S2L, s_r2)
    for _ in range(3):
        arrived(YR.at[pl.ds(0, 1)], s_ry)
    arrived(SCR.at[pl.ds(0, SEQ - 1)], s_sc)
    for result in results:
        result.wait()


def on_device(patch_embed, perturbation, target, ln_gain, ln_bias, w_qkv, w_out, radius, step_size):
    anywhere = pl.BlockSpec(memory_space=pl.ANY)
    dma = pltpu.SemaphoreType.DMA
    V = pltpu.VMEM
    scratch = [
        V(patch_embed.shape, BF16),
        V(perturbation.shape, F32),
        V(target.shape, BF16),
        V(ln_gain.shape, F32),
        V(ln_bias.shape, F32),
        pltpu.SMEM(radius.shape, F32),
        pltpu.SMEM(step_size.shape, F32),
        V((4, 4, 2, BLOCK, WIDTH), BF16),
        V((4, CHUNK, WIDTH // 2), BF16),
        V((6, PAD, WIDTH), BF16),
        V((6, PAD, WIDTH), BF16),
        V((PLANES, 2 * PAD, WIDTH), BF16),
        V((IMAGES, BLOCK, WIDTH), F32),
        V((IMAGES, BLOCK, PAD), F32),
        V((IMAGES, BLOCK, WIDTH), BF16),
        V((2, 1024, PAD), BF16),
        V((2, 1024, PAD), BF16),
        V((2, 1024, PAD), BF16),
        V((2, 4, 8, BLOCK, PAD), BF16),
        V((4, 8, PACKED, PAD), BF16),
        V((SEQ, PACKED, PAD), BF16),
        V((2, 8, 1024), F32),
        V((2, 8, 1024), F32),
        V((4, 8, PACKED, PAD), BF16),
        V((32, PACKED, PAD), BF16),
        V((2, 1024, PAD), BF16),
        V((2, PAD, 1024), F32),
        V((2, 4, 4, BLOCK, 6 * PAD), BF16),
        V((4, 4, BLOCK, 6 * PAD), BF16),
        V((IMAGES, BLOCK, WIDTH), F32),
        V((IMAGES * BLOCK, WIDTH), BF16),
        V((NSTEPS, 4, 4, BLOCK, NB), F32),
        V((NSTEPS, 2, 4, 16, NB), BF16),
        V((NSTEPS, 4, 16, NB), BF16),
        V((NSTEPS, 4, 16, NB), BF16),
        V((NSTEPS, 4, BLOCK, NB), BF16),
        V((NSTEPS, 4, BLOCK, NB), BF16),
        V((NSTEPS, 4, BLOCK, NB), BF16),
        V((NSTEPS, 4, BLOCK, NB), BF16),
        V((NSTEPS, 4, BLOCK, NB), BF16),
        V((4, NSTEPS, BLOCK, NB), BF16),
        V((8, PAD), F32),
        V((SEQ, 8, PAD), F32),
        V((PAD,), F32),
        V((PAD,), F32),
        dma((7,)), dma((IMAGES,)), dma((2,)), dma, dma((4,)),
        dma, dma((CHUNKS,)), dma, dma((CHUNKS,)), dma((CHUNKS,)), dma((CHUNKS,)),
        dma, dma((3,)), dma, dma((4,)), dma((4,)), dma((4,)), dma((4,)),
        dma, dma((16,)),
        dma, dma((8,)), dma((2, 3)), dma, dma((8,)), dma((8,)), dma((8,)), dma, dma((8,)), dma,
        dma, dma,
        dma, dma, dma, dma,
        dma, dma((2, 5)),
        dma, dma((NSTEPS,)), dma((NSTEPS,)),
        dma, dma((NSTEPS,)), dma((NSTEPS,)),
        dma, dma((3, NSTEPS)),
        dma, dma,
    ]
    gradient, shrink, factor = pl.pallas_call(
        kernel,
        out_shape=(
            jax.ShapeDtypeStruct(perturbation.shape, F32),
            jax.ShapeDtypeStruct((PAD,), F32),
            jax.ShapeDtypeStruct((PAD,), F32),
        ),
        in_specs=[anywhere] * 9,
        out_specs=(anywhere,) * 3,
        scratch_shapes=scratch,
        compiler_params=pltpu.CompilerParams(
            collective_id=0, has_side_effects=True, vmem_limit_bytes=62 * 1024 * 1024
        ),
    )(
        patch_embed,
        perturbation,
        target,
        ln_gain,
        ln_bias,
        w_qkv.reshape(12, CHUNK, WIDTH),
        w_out.reshape(2 * HD, WIDTH),
        radius,
        step_size,
    )
    return perturbation * shrink[:IMAGES, None, None] + factor[:IMAGES, None, None] * gradient


def solution(mesh):
    placed = (
        P("head", "seq", None),
        P("head", "seq", None),
        P("head", "seq", None),
        P(),
        P(),
        P("head", None, None),
        P("head", None, None),
        P(),
        P(),
    )
    return jax.shard_map(
        on_device, mesh=mesh, in_specs=placed, out_specs=P("head", "seq", None), check_vma=False
    )
```

```python
import functools
import math

import jax
import jax.numpy as jnp
from jax import lax
from jax.experimental import pallas as pl
from jax.experimental.pallas import tpu as pltpu
from jax.sharding import PartitionSpec as P

norm_epsilon = 1e-06
layer_epsilon = 1e-06

F32 = jnp.float32
BF16 = jnp.bfloat16
NT = (((1,), (1,)), ((), ()))
NN = (((1,), (0,)), ((), ()))
TN = (((0,), (0,)), ((), ()))

IMAGES = 4
ROWS = 4
COLS = 4
PLANES = 8
SEQ = 32
BLOCK = 32
WIDTH = 1280
HD = 80
PACKED = 40
PAD = 128
CHUNK = 40
NB = 256
NSTEPS = WIDTH // NB
CHUNKS = 6
TILE = 256


def dot(a, b, dims):
    return lax.dot_general(a, b, dims, preferred_element_type=F32)


def lane_of(value):
    return lax.broadcasted_iota(jnp.int32, value.shape, value.ndim - 1)


def pack_rest(rest):
    groups = rest.reshape(-1, 4, 8, PAD)
    packed = groups[:, 0].reshape(-1, PAD)
    lane = lane_of(packed)
    for g in range(1, 4):
        turned = pltpu.roll(groups[:, g].reshape(-1, PAD), 32 * g, 1)
        packed = jnp.where(lane >= 32 * g, turned, packed)
    return packed.reshape(-1, 8, PAD)


def unpack_rest(packed, lane):
    flat = packed.reshape(-1, PAD)
    groups = [
        pltpu.roll(flat, (PAD + lane - 32 * g) % PAD, 1).reshape(-1, 1, 8, PAD) for g in range(4)
    ]
    return jnp.concatenate(groups, axis=1).reshape(-1, PAD)


def shard_offset(x, c):
    other = 8 - x - 4 * (1 - (x + 3) // 4)
    return (1 - c) * x + c * other


def kernel(
    pe_in, pert_in, tgt_in, gain_in, bias_in, w_own, wo_own, rad_in, stp_in, grad_out, shrink_out, factor_out,
    pe, pert, tgt, gain, bias, rad, stp,
    H, RB, Wp, W2, WO, normed, inv, HS, Q, K, V, O, OS, OR, LSE, DOT, GS, GO, GH, GQ, GP, GP2,
    RES, RESB, PF, PB, R1L, R1R, S2L, S2R, R2L, R2R, YS, YR, SC, SCR, SHRINK, FACTOR,
    l_in, l_out, l_res, s_rb, r_rb, s_wz, r_wz, s_wy, r_wyl, r_wyr, r_wyy, s_hy, r_hy, s_hx, r_hxl, r_hxr, r_hxy, r_hxz,
    s_hd, r_hd, s_wo, r_wo, r_wof, s_woy, r_wol, r_wor, r_woz, s_wod, r_wod, l_wo, s_wd, r_wd, s_oa, r_oa, s_ga, r_ga,
    s_gp, r_gp, s_r1, r_r1l, r_r1r, s_r2, r_r2l, r_r2r, s_ry, r_ry, s_sc, r_sc,
):
    s = lax.axis_index("seq")
    z = lax.axis_index("head")
    y = s // 8
    x = (s // 2) % 4
    c = s % 2
    k8 = s % 8

    def at(yy, xx, cc):
        return (yy * 4 + xx) * 2 + cc

    right = at(y, (x + 1) % 4, c)
    left = at(y, (x + 3) % 4, c)
    down = at((y + 1) % 4, x, c)
    up = at((y + 3) % 4, x, c)
    partner = at(y, x, 1 - c)

    def send(src, dst, ssem, rsem, **where):
        copy = pltpu.make_async_remote_copy(
            src_ref=src, dst_ref=dst, send_sem=ssem, recv_sem=rsem,
            device_id=where, device_id_type=pl.DeviceIdType.MESH,
        )
        copy.start()

    def arrived(ref, sem):
        pltpu.make_async_copy(ref, ref, sem).wait()

    loads = [
        pltpu.make_async_copy(src, dst, l_in.at[i])
        for i, (src, dst) in enumerate(
            ((pe_in, pe), (pert_in, pert), (gain_in, gain), (bias_in, bias), (tgt_in, tgt),
             (rad_in, rad), (stp_in, stp))
        )
    ]
    for load in loads:
        load.start()

    barrier = pltpu.get_barrier_semaphore()

    for d in range(1, SEQ):
        pl.semaphore_signal(
            barrier, inc=1, device_id={"seq": (s + d) % SEQ}, device_id_type=pl.DeviceIdType.MESH
        )
    for d in range(1, PLANES):
        pl.semaphore_signal(
            barrier, inc=1, device_id={"head": (z + d) % PLANES},
            device_id_type=pl.DeviceIdType.MESH,
        )

    own_wo = pltpu.make_async_copy(wo_own, WO.at[z, pl.ds(0, 2 * HD)], l_wo)
    own_wo.start()

    def normalize(image):
        mixed = pe[image].astype(F32) + pert[image]
        rounded = mixed.astype(BF16).astype(F32)
        center = rounded - jnp.mean(rounded, axis=-1, keepdims=True)
        variance = jnp.mean(center * center, axis=-1, keepdims=True)
        inverse = lax.rsqrt(variance + layer_epsilon)
        return mixed, center * inverse, inverse

    def layer_norm(image):
        _, unit, _ = normalize(image)
        return (unit * gain[...].reshape(1, WIDTH) + bias[...].reshape(1, WIDTH)).astype(BF16)

    for load in loads[:4]:
        load.wait()

    @pl.loop(1, ROWS)
    def _(d):
        image = (y + d) % 4
        HS[image] = layer_norm(image)

    H[y, x, c] = layer_norm(y)

    pl.semaphore_wait(barrier, SEQ - 1 + PLANES - 1)

    offset = shard_offset(x, c)
    target = (z + 8 - offset) % 8

    half_width = WIDTH // 2

    def ways(plane):
        odd = plane % 2
        place = odd * y + (1 - odd) * x
        return place, odd * down + (1 - odd) * right, odd * up + (1 - odd) * left

    def piece(ref, place, cc):
        rows = pl.ds(pl.multiple_of(CHUNK * place, 8), CHUNK)
        lanes = pl.ds(pl.multiple_of(cc * half_width, PAD), half_width)
        return ref.at[rows, lanes]

    def half_shard(plane, cc):
        lanes = pl.ds(pl.multiple_of(cc * half_width, PAD), half_width)
        return WO.at[plane, pl.ds(0, 2 * HD), lanes]

    place, _, _ = ways(z)
    for d in (1, 7):
        send(piece(wo_own, place, c), piece(WO.at[z], place, c), s_wo, r_wo.at[d], head=(z + d) % 8)

    def chunk(yy, q):
        u = 3 * yy + q % 3
        rows = pl.ds(pl.multiple_of(CHUNK * (u % 2), 8), CHUNK)
        return Wp.at[u // 2, rows, pl.ds((q // 3) * half_width, half_width)]

    def source(q):
        return w_own.at[3 * y + q % 3, :, pl.ds((q // 3) * half_width, half_width)]

    between = {0: (0, 2), 1: (1, 6), 3: (2, 2), 4: (3, 6)}

    for q in range(CHUNKS):
        @pl.when(offset == 0)
        def _():
            pltpu.make_async_copy(source(q), chunk(y, q), r_wz.at[q]).start()

        if q in between:
            slot, hop = between[q]

            @pl.when(offset == 4)
            def _():
                send(source(q), RB.at[slot], s_wz, r_rb.at[slot], head=(z + hop) % 8)

            @pl.when((offset != 0) & (offset != 4))
            def _():
                send(source(q), chunk(y, q), s_wz, r_wz.at[q], head=target)
        else:
            @pl.when(offset != 0)
            def _():
                send(source(q), chunk(y, q), s_wz, r_wz.at[q], head=target)

    def pass_on(q):
        slot, hop = between[q]

        @pl.when(offset == 4)
        def _():
            arrived(RB.at[slot], r_rb.at[slot])
            send(RB.at[slot], chunk(y, q), s_rb, r_wz.at[q], head=(z + hop) % 8)

    @pl.loop(1, ROWS)
    def _(d):
        image = (y + d) % 4
        send(HS.at[image], H.at[y, x, c], s_hy, r_hy.at[d - 1], seq=at(image, x, c))

    def spread(d):
        yy = (y + d) % 4
        block = H.at[yy, x, c]
        send(block, block, s_hx, r_hxl.at[d], seq=right)
        send(block, block, s_hx, r_hxr.at[d], seq=left)
        send(block, block, s_hd, r_hd.at[d * 4], seq=partner)

    def relay(d):
        yy = (y + d) % 4
        from_left = H.at[yy, (x + 3) % 4, c]
        arrived(from_left, r_hxl.at[d])
        upper = H.at[yy, (x + 3) % 4, c, pl.ds(0, 16)]
        send(upper, upper, s_hx, r_hxy.at[d], seq=right)
        send(from_left, from_left, s_hd, r_hd.at[d * 4 + 1], seq=partner)
        from_right = H.at[yy, (x + 1) % 4, c]
        arrived(from_right, r_hxr.at[d])
        lower = H.at[yy, (x + 1) % 4, c, pl.ds(16, 16)]
        send(lower, lower, s_hx, r_hxz.at[d], seq=left)
        send(from_right, from_right, s_hd, r_hd.at[d * 4 + 2], seq=partner)

    def from_row(d):
        arrived(H.at[(y + d) % 4, x, c], r_hy.at[3 - d])
        spread(d)

    def round_column(j):
        arrived(chunk(y, j), r_wz.at[j])
        send(chunk(y, j), chunk(y, j), s_wy, r_wyl.at[j], seq=down)
        send(chunk(y, j), chunk(y, j), s_wy, r_wyr.at[j], seq=up)

    def wo_chain(step):
        for d, ahead, there, last in ((step, 1, step + 1, 4), (8 - step, 7, 7 - step, 5)):
            if step == 4 and ahead == 7:
                continue
            plane = (z + 8 - d) % 8
            place, _, _ = ways(plane)
            got = piece(WO.at[plane], place, c)
            arrived(got, r_wo.at[d])
            if d != last:
                send(got, got, s_wo, r_wo.at[there], head=(z + ahead) % 8)

    def wo_give():
        place, _, _ = ways(z)
        for i, d in enumerate((1, 7)):
            for part in range(3):
                spot = (place + 1 + part) % 4
                send(
                    piece(wo_own, spot, c), piece(WO.at[z], spot, c), s_wo, r_wof.at[i, part],
                    head=(z + d) % 8,
                )

    def wo_near():
        for i, d in enumerate((1, 7)):
            plane = (z + 8 - d) % 8
            place, _, _ = ways(plane)
            for part in range(3):
                arrived(piece(WO.at[plane], (place + 1 + part) % 4, c), r_wof.at[i, part])
            send(half_shard(plane, c), half_shard(plane, c), s_wod, r_wod.at[d], seq=partner)

    def wo_first(d):
        plane = (z + 8 - d) % 8
        place, after, before = ways(plane)
        got = piece(WO.at[plane], place, c)
        send(got, got, s_woy, r_wol.at[d], seq=after)
        send(got, got, s_woy, r_wor.at[d], seq=before)
        send(got, got, s_wod, r_wod.at[d], seq=partner)

    def wo_second(d):
        plane = (z + 8 - d) % 8
        place, after, before = ways(plane)
        shard = WO.at[plane]
        lower, upper = piece(shard, (place + 3) % 4, c), piece(shard, (place + 1) % 4, c)
        arrived(lower, r_wol.at[d])
        arrived(upper, r_wor.at[d])
        send(lower, lower, s_wod, r_wod.at[d], seq=partner)
        send(upper, upper, s_wod, r_wod.at[d], seq=partner)
        turn = (plane // 2) % 2

        @pl.when(turn == 0)
        def _():
            send(lower, lower, s_woy, r_woz.at[d], seq=after)

        @pl.when(turn == 1)
        def _():
            send(upper, upper, s_woy, r_woz.at[d], seq=before)

    def wo_third(d):
        plane = (z + 8 - d) % 8
        place, _, _ = ways(plane)
        got = piece(WO.at[plane], (place + 2) % 4, c)
        arrived(got, r_woz.at[d])
        send(got, got, s_wod, r_wod.at[d], seq=partner)

    yu, yd, yo = (y + 3) % 4, (y + 1) % 4, (y + 2) % 4

    def relay_column(q):
        arrived(chunk(yu, q), r_wyl.at[q])
        arrived(chunk(yd, q), r_wyr.at[q])
        if q % 2 == 0:
            send(chunk(yu, q), chunk(yu, q), s_wy, r_wyy.at[q], seq=down)
        else:
            send(chunk(yd, q), chunk(yd, q), s_wy, r_wyy.at[q], seq=up)

    def far_column(d):
        yy, xx = (y + d) % 4, (x + 2) % 4
        arrived(H.at[yy, xx, c, pl.ds(0, 16)], r_hxy.at[d])
        arrived(H.at[yy, xx, c, pl.ds(16, 16)], r_hxz.at[d])
        send(H.at[yy, xx, c], H.at[yy, xx, c], s_hd, r_hd.at[d * 4 + 3], seq=partner)

    spread(0)

    @pl.loop(0, 6)
    def _(t):
        Wp[t, HD:PAD, :] = jnp.zeros((PAD - HD, WIDTH), BF16)

    @pl.loop(0, PLANES)
    def _(t):
        WO[t, 2 * HD : 2 * PAD, :] = jnp.zeros((2 * (PAD - HD), WIDTH), BF16)

    for load in loads[4:]:
        load.wait()

    @pl.loop(0, IMAGES)
    def _(image):
        mixed, unit, inverse = normalize(image)
        normed[image] = unit
        inv[image] = jnp.broadcast_to(inverse, (BLOCK, PAD))
        RES[image] = mixed - tgt[image].astype(F32)

    from_row(1)
    relay(0)
    wo_chain(1)
    from_row(3)
    pass_on(0)
    pass_on(1)
    from_row(2)
    round_column(0)
    round_column(1)
    pass_on(3)
    pass_on(4)
    relay(1)
    round_column(2)
    relay_column(0)
    relay(3)
    wo_chain(2)
    relay_column(1)
    relay(2)
    round_column(3)
    relay_column(2)
    round_column(4)
    far_column(0)
    round_column(5)
    wo_give()
    relay_column(3)
    wo_chain(3)
    wo_first(2)
    wo_first(6)
    far_column(1)
    relay_column(4)
    far_column(3)
    relay_column(5)
    far_column(2)

    for q in range(CHUNKS):
        arrived(chunk(yo, q), r_wyy.at[q])

    send(Wp, W2, s_wd, r_wd, seq=partner)
    wo_chain(4)
    for d in (3, 5, 4):
        wo_first(d)

    @pl.loop(0, ROWS)
    def _(d):
        yy = (y + d) % 4
        arrived(H.at[yy, x, 1 - c], r_hd.at[d * 4])
        arrived(H.at[yy, (x + 3) % 4, 1 - c], r_hd.at[d * 4 + 1])
        arrived(H.at[yy, (x + 1) % 4, 1 - c], r_hd.at[d * 4 + 2])
        arrived(H.at[yy, (x + 2) % 4, 1 - c], r_hd.at[d * 4 + 3])

    @pl.loop(0, 2)
    def _(t):
        rows = pl.ds(pl.multiple_of(t * 512, 512), 512)
        tokens = H[pl.ds(2 * t, 2)].reshape(512, WIDTH)
        packed = dot(tokens, Wp[...].reshape(6 * PAD, WIDTH), NT).astype(BF16)
        for h in range(2):
            Q[h, rows] = packed[:, (3 * h) * PAD : (3 * h + 1) * PAD]
            K[h, rows] = packed[:, (3 * h + 1) * PAD : (3 * h + 2) * PAD]
            V[h, rows] = packed[:, (3 * h + 2) * PAD : (3 * h + 3) * PAD]

    scale = 1.0 / math.sqrt(HD)
    scale2 = scale * math.log2(math.e)

    wo_near()
    for d in (2, 6):
        wo_second(d)

    @pl.loop(0, 4)
    def _(step):
        row = (y + 3 - step) % 4

        @pl.when(step == 3)
        def _():
            for d in (3, 5, 4):
                wo_second(d)

        rows = pl.ds(pl.multiple_of(row * TILE, TILE), TILE)
        parts = []
        for h in range(2):
            scores = dot(Q[h, rows], K[h], NT)
            top = jnp.max(scores, axis=-1, keepdims=True) * scale2
            grown = jnp.exp2(scores * scale2 - top)
            total = jnp.sum(grown, axis=-1, keepdims=True)
            part = dot(grown.astype(BF16), V[h], NN) * (1.0 / total)
            parts.append(part)
            O[h, row] = part.astype(BF16).reshape(8, BLOCK, PAD)
            column = jnp.broadcast_to(top + jnp.log2(total), (TILE, PAD))
            LSE[h, :, rows] = jnp.transpose(column)[0:8]

        turned = pltpu.roll(parts[1], HD, 1)
        whole = jnp.where(lane_of(turned) < HD, parts[0], turned)
        OS[row, :, 0:BLOCK] = whole.astype(BF16).reshape(8, BLOCK, PAD)
        OS[row, :, BLOCK:PACKED] = pack_rest(turned).astype(BF16)

        def give(turn):
            k = (k8 + turn) % 8
            send(OS.at[row, k], OR.at[s], s_oa, r_oa, seq=row * 8 + k)

        for turn in (4, 5, 3, 6, 2, 7, 1):
            give(turn)

        @pl.when(step != 3)
        def _():
            give(0)

    OR[s] = OS[y, k8]

    for d in (2, 6, 3, 5, 4):
        wo_third(d)
    own_wo.wait()

    arrived(OR.at[pl.ds(0, SEQ - 1)], r_oa)

    @pl.loop(0, 4)
    def _(turn):
        pair = [(k, shard_offset(k // 2, k % 2)) for k in (2 * turn, (2 * turn + 3) % 8)]
        for _, away in pair:
            @pl.when(away != 0)
            def _(away=away):
                arrived(half_shard((z + away) % 8, 1 - c), r_wod.at[(8 - away) % 8])

        branch = jnp.zeros((128, WIDTH), F32)
        for k, away in pair:
            rest = jnp.concatenate([OR[i * 8 + k, BLOCK:PACKED] for i in range(IMAGES)], axis=0)
            rest = unpack_rest(rest.astype(F32), 0)
            rest = jnp.where(lane_of(rest) < 32, rest, 0.0).astype(BF16)
            whole = jnp.concatenate([OR[i * 8 + k, 0:BLOCK] for i in range(IMAGES)], axis=0)
            heads = jnp.concatenate([whole, rest], axis=-1)
            branch = branch + dot(heads, WO[(z + away) % 8], NN)
        RES[...] += branch.reshape(IMAGES, BLOCK, WIDTH)

    RESB[...] = RES[...].reshape(128, WIDTH).astype(BF16)

    @pl.loop(0, 4)
    def _(turn):
        xx = (x + 3 - turn) % 4
        for cc in range(2):
            back = dot(RESB[...], WO[(z + shard_offset(xx, cc)) % 8], NT)
            GS[:, 2 * xx + cc, 0:BLOCK] = (
                back[:, 0:PAD].astype(BF16).reshape(IMAGES, BLOCK, PAD)
            )
            GS[:, 2 * xx + cc, BLOCK:PACKED] = pack_rest(back[:, PAD : 2 * PAD]).astype(BF16)

        def give(away, cc):
            i, k = (y + away) % 4, 2 * xx + cc
            send(GS.at[i, k], GO.at[s], s_ga, r_ga, seq=i * 8 + k)

        for away in (2, 1, 3):
            for cc in range(2):
                give(away, cc)

        for cc in range(2):
            @pl.when(2 * xx + cc != k8)
            def _(cc=cc):
                give(0, cc)

    GO[s] = GS[y, k8]

    arrived(GO.at[pl.ds(0, SEQ - 1)], r_ga)

    @pl.loop(0, 4)
    def _(row):
        blocks = pl.ds(row * 8, 8)
        rows = pl.ds(pl.multiple_of(row * TILE, TILE), TILE)
        whole = GO[blocks, 0:BLOCK].astype(F32).reshape(TILE, PAD)
        rest = unpack_rest(GO[blocks, BLOCK:PACKED].astype(F32), PAD - HD)
        lane = lane_of(whole)
        turned = pltpu.roll(whole, PAD - HD, 1)
        GH[0, rows] = jnp.where(lane < HD, whole, 0.0).astype(BF16)
        GH[1, rows] = jnp.where(
            lane < PAD - HD, turned, jnp.where(lane < HD, rest, 0.0)
        ).astype(BF16)

    for h in range(2):
        products = GH[h].astype(F32) * O[h].reshape(1024, PAD).astype(F32)
        DOT[h] = jnp.broadcast_to(
            jnp.sum(jnp.transpose(products), axis=0, keepdims=True), (8, 1024)
        )

    GQ[...] = jnp.zeros((2, PAD, 1024), F32)

    def store(block_row, h, kind, value):
        parts = value.astype(BF16).reshape(4, 2, BLOCK, PAD)
        t = h * 3 + kind
        for cc in range(2):
            GP[cc, block_row, :, :, t * PAD : (t + 1) * PAD] = parts[:, cc]

    @pl.loop(0, 4)
    def _(row):
        rows = pl.ds(pl.multiple_of(row * TILE, TILE), TILE)
        for h in range(2):
            queries = Q[h]
            grads = GH[h]
            scores = dot(K[h, rows], queries, NT)
            weights = jnp.exp2(scores * scale2 - LSE[h, 0:1])
            grad_values = dot(weights.astype(BF16), grads, NN)
            grad_weights = dot(V[h, rows], grads, NT)
            grad_scores = (weights * (grad_weights - DOT[h, 0:1])).astype(BF16)
            grad_keys = dot(grad_scores, queries, NN) * scale
            grad_query = dot(K[h, rows], grad_scores, TN)

            GQ[h] += grad_query

            store(row, h, 1, grad_keys)
            store(row, h, 2, grad_values)

        for h in range(2):
            lanes = pl.ds((h * 3 + 1) * PAD, 2 * PAD)
            send(
                GP.at[1 - c, row, :, :, lanes], GP2.at[row, :, :, lanes], s_gp, r_gp.at[h, row],
                seq=partner,
            )

    for h in range(2):
        for r in range(4):
            store(r, h, 0, jnp.transpose(GQ[h, :, r * TILE : (r + 1) * TILE]) * scale)
        lanes = pl.ds(h * 3 * PAD, PAD)
        send(GP.at[1 - c, :, :, :, lanes], GP2.at[:, :, :, lanes], s_gp, r_gp.at[h, 4], seq=partner)

    arrived(W2, r_wd)
    for h in range(2):
        for r in range(4):
            arrived(GP2.at[r, :, :, pl.ds((h * 3 + 1) * PAD, 2 * PAD)], r_gp.at[h, r])
        arrived(GP2.at[:, :, :, pl.ds(h * 3 * PAD, PAD)], r_gp.at[h, 4])

    xr, xl, xo = (x + 1) % 4, (x + 3) % 4, (x + 2) % 4

    @pl.loop(0, NSTEPS)
    def _(n):
        lanes = pl.ds(pl.multiple_of(n * NB, NB), NB)
        mine = GP[c].reshape(512, 6 * PAD)
        other = GP2[...].reshape(512, 6 * PAD)
        part = dot(mine, Wp[:, :, lanes].reshape(6 * PAD, NB), NN)
        part = part + dot(other, W2[:, :, lanes].reshape(6 * PAD, NB), NN)
        PF[n] = part.reshape(4, 4, BLOCK, NB)
        PB[n, 0] = PF[n, :, xo, 0:16].astype(BF16)
        PB[n, 1] = PF[n, :, xo, 16:32].astype(BF16)
        send(PB.at[n, 0], R1L.at[n], s_r1, r_r1l.at[n], seq=right)
        send(PB.at[n, 1], R1R.at[n], s_r1, r_r1r.at[n], seq=left)

    @pl.loop(0, NSTEPS)
    def _(n):
        arrived(R1L.at[n], r_r1l.at[n])
        S2R[n, :, 0:16] = (PF[n, :, xr, 0:16] + R1L[n].astype(F32)).astype(BF16)
        S2R[n, :, 16:32] = PF[n, :, xr, 16:32].astype(BF16)
        send(S2R.at[n], R2L.at[n], s_r2, r_r2l.at[n], seq=right)
        arrived(R1R.at[n], r_r1r.at[n])
        S2L[n, :, 16:32] = (PF[n, :, xl, 16:32] + R1R[n].astype(F32)).astype(BF16)
        S2L[n, :, 0:16] = PF[n, :, xl, 0:16].astype(BF16)
        send(S2L.at[n], R2R.at[n], s_r2, r_r2r.at[n], seq=left)

    @pl.loop(0, NSTEPS)
    def _(n):
        arrived(R2L.at[n], r_r2l.at[n])
        arrived(R2R.at[n], r_r2r.at[n])
        total = PF[n, :, x] + R2L[n].astype(F32) + R2R[n].astype(F32)
        YS[n] = total.astype(BF16)
        for d in (2, 1, 3):
            send(
                YS.at[n, (y + d) % 4], YR.at[y, n], s_ry, r_ry.at[d - 1, n],
                seq=at((y + d) % 4, x, c),
            )

    for n in range(NSTEPS):
        YR[y, n] = YS[n, y]

    @pl.loop(0, NSTEPS)
    def _(n):
        for d in range(1, 4):
            arrived(YR.at[(y + d) % 4, n], r_ry.at[3 - d, n])

    lane = lax.broadcasted_iota(jnp.int32, (8, PAD), 1)
    line = lax.broadcasted_iota(jnp.int32, (8, PAD), 0)

    def total_of(value):
        return jnp.sum(jnp.sum(value, axis=0, keepdims=True), axis=1, keepdims=True)

    sums = jnp.zeros((8, PAD), F32)
    for i in range(IMAGES):
        back = jnp.concatenate([YR[i, n] for n in range(NSTEPS)], axis=-1)
        scaled = back.astype(F32) * gain[...].reshape(1, WIDTH)
        unit = normed[i]
        first = jnp.mean(scaled, axis=-1, keepdims=True)
        second = jnp.mean(scaled * unit, axis=-1, keepdims=True)
        gradient = RES[i] + (scaled - first - unit * second) * inv[i][:, 0:1]
        RES[i] = gradient
        pltpu.make_async_copy(RES.at[i], grad_out.at[i], l_out.at[i]).start()
        current = pert[i]
        for j, value in enumerate((gradient * gradient, current * gradient, current * current)):
            sums = jnp.where((line == i) & (lane == j), total_of(value), sums)
    SC[...] = sums
    SCR[s] = sums

    for d in (18, 20, 22, 16, 17, 19, 21, 23, *range(8, 16), *range(24, 32), *range(1, 8)):
        send(SC, SCR.at[s], s_sc, r_sc, seq=(s + d) % SEQ)

    arrived(SCR.at[pl.ds(0, SEQ - 1)], r_sc)
    sums = jnp.sum(SCR[...], axis=0)
    column = lax.broadcasted_iota(jnp.int32, (8, 1), 0)
    step_of, radius_of = jnp.ones((8, 1), F32), jnp.ones((8, 1), F32)
    for i in range(IMAGES):
        step_of = jnp.where(column == i, stp[z * IMAGES + i], step_of)
        radius_of = jnp.where(column == i, rad[z * IMAGES + i], radius_of)
    grad_square, cross, own = sums[:, 0:1], sums[:, 1:2], sums[:, 2:3]
    factor = step_of / jnp.sqrt(grad_square + norm_epsilon)
    stepped_square = own + 2.0 * factor * cross + factor * factor * grad_square
    shrink = jnp.minimum(1.0, radius_of / jnp.sqrt(stepped_square + norm_epsilon))
    shrink_row, factor_row = jnp.zeros((1, PAD), F32), jnp.zeros((1, PAD), F32)
    for i in range(IMAGES):
        shrink_row = jnp.where(lane[0:1] == i, shrink[i : i + 1], shrink_row)
        factor_row = jnp.where(lane[0:1] == i, (factor * shrink)[i : i + 1], factor_row)
    SHRINK[...] = shrink_row.reshape(PAD)
    FACTOR[...] = factor_row.reshape(PAD)
    results = [
        pltpu.make_async_copy(SHRINK, shrink_out, l_res.at[0]),
        pltpu.make_async_copy(FACTOR, factor_out, l_res.at[1]),
    ]
    for result in results:
        result.start()
    for i in range(IMAGES):
        pltpu.make_async_copy(RES.at[i], grad_out.at[i], l_out.at[i]).wait()

    @pl.when(offset != 0)
    def _():
        for q in range(CHUNKS):
            arrived(source(q), s_wz)

    @pl.when(offset == 4)
    def _():
        arrived(RB, s_rb)

    for q in range(CHUNKS):
        for _ in range(3):
            arrived(source(q), s_wy)
    arrived(HS.at[pl.ds(0, 3)], s_hy)
    arrived(H.at[0, :, :].reshape(8, BLOCK, WIDTH), s_hx)
    arrived(H.at[0, pl.ds(0, 2)].reshape(4, BLOCK, WIDTH), s_hx)
    arrived(H.at[pl.ds(0, 2)].reshape(16, BLOCK, WIDTH), s_hd)
    arrived(Wp, s_wd)
    for d in range(1, PLANES):
        arrived(piece(wo_own, y, c), s_wo)
        if d in (1, 7):
            for _ in range(3):
                arrived(piece(wo_own, y, c), s_wo)
        else:
            for _ in range(3):
                arrived(piece(wo_own, y, c), s_woy)
        arrived(half_shard(z, c), s_wod)
    arrived(OR.at[pl.ds(0, SEQ - 1)], s_oa)
    arrived(GO.at[pl.ds(0, SEQ - 1)], s_ga)
    arrived(GP2, s_gp)
    arrived(PB, s_r1)
    arrived(S2R, s_r2)
    arrived(S2L, s_r2)
    for _ in range(3):
        arrived(YR.at[pl.ds(0, 1)], s_ry)
    arrived(SCR.at[pl.ds(0, SEQ - 1)], s_sc)
    for result in results:
        result.wait()


def on_device(patch_embed, perturbation, target, ln_gain, ln_bias, w_qkv, w_out, radius, step_size):
    anywhere = pl.BlockSpec(memory_space=pl.ANY)
    dma = pltpu.SemaphoreType.DMA
    V = pltpu.VMEM
    scratch = [
        V(patch_embed.shape, BF16),
        V(perturbation.shape, F32),
        V(target.shape, BF16),
        V(ln_gain.shape, F32),
        V(ln_bias.shape, F32),
        pltpu.SMEM(radius.shape, F32),
        pltpu.SMEM(step_size.shape, F32),
        V((4, 4, 2, BLOCK, WIDTH), BF16),
        V((4, CHUNK, WIDTH // 2), BF16),
        V((6, PAD, WIDTH), BF16),
        V((6, PAD, WIDTH), BF16),
        V((PLANES, 2 * PAD, WIDTH), BF16),
        V((IMAGES, BLOCK, WIDTH), F32),
        V((IMAGES, BLOCK, PAD), F32),
        V((IMAGES, BLOCK, WIDTH), BF16),
        V((2, 1024, PAD), BF16),
        V((2, 1024, PAD), BF16),
        V((2, 1024, PAD), BF16),
        V((2, 4, 8, BLOCK, PAD), BF16),
        V((4, 8, PACKED, PAD), BF16),
        V((SEQ, PACKED, PAD), BF16),
        V((2, 8, 1024), F32),
        V((2, 8, 1024), F32),
        V((4, 8, PACKED, PAD), BF16),
        V((32, PACKED, PAD), BF16),
        V((2, 1024, PAD), BF16),
        V((2, PAD, 1024), F32),
        V((2, 4, 4, BLOCK, 6 * PAD), BF16),
        V((4, 4, BLOCK, 6 * PAD), BF16),
        V((IMAGES, BLOCK, WIDTH), F32),
        V((IMAGES * BLOCK, WIDTH), BF16),
        V((NSTEPS, 4, 4, BLOCK, NB), F32),
        V((NSTEPS, 2, 4, 16, NB), BF16),
        V((NSTEPS, 4, 16, NB), BF16),
        V((NSTEPS, 4, 16, NB), BF16),
        V((NSTEPS, 4, BLOCK, NB), BF16),
        V((NSTEPS, 4, BLOCK, NB), BF16),
        V((NSTEPS, 4, BLOCK, NB), BF16),
        V((NSTEPS, 4, BLOCK, NB), BF16),
        V((NSTEPS, 4, BLOCK, NB), BF16),
        V((4, NSTEPS, BLOCK, NB), BF16),
        V((8, PAD), F32),
        V((SEQ, 8, PAD), F32),
        V((PAD,), F32),
        V((PAD,), F32),
        dma((7,)), dma((IMAGES,)), dma((2,)), dma, dma((4,)),
        dma, dma((CHUNKS,)), dma, dma((CHUNKS,)), dma((CHUNKS,)), dma((CHUNKS,)),
        dma, dma((3,)), dma, dma((4,)), dma((4,)), dma((4,)), dma((4,)),
        dma, dma((16,)),
        dma, dma((8,)), dma((2, 3)), dma, dma((8,)), dma((8,)), dma((8,)), dma, dma((8,)), dma,
        dma, dma,
        dma, dma, dma, dma,
        dma, dma((2, 5)),
        dma, dma((NSTEPS,)), dma((NSTEPS,)),
        dma, dma((NSTEPS,)), dma((NSTEPS,)),
        dma, dma((3, NSTEPS)),
        dma, dma,
    ]
    gradient, shrink, factor = pl.pallas_call(
        kernel,
        out_shape=(
            jax.ShapeDtypeStruct(perturbation.shape, F32),
            jax.ShapeDtypeStruct((PAD,), F32),
            jax.ShapeDtypeStruct((PAD,), F32),
        ),
        in_specs=[anywhere] * 9,
        out_specs=(anywhere,) * 3,
        scratch_shapes=scratch,
        compiler_params=pltpu.CompilerParams(
            collective_id=0, has_side_effects=True, vmem_limit_bytes=62 * 1024 * 1024
        ),
    )(
        patch_embed,
        perturbation,
        target,
        ln_gain,
        ln_bias,
        w_qkv.reshape(12, CHUNK, WIDTH),
        w_out.reshape(2 * HD, WIDTH),
        radius,
        step_size,
    )
    return perturbation * shrink[:IMAGES, None, None] + factor[:IMAGES, None, None] * gradient


def solution(mesh):
    placed = (
        P("head", "seq", None),
        P("head", "seq", None),
        P("head", "seq", None),
        P(),
        P(),
        P("head", None, None),
        P("head", None, None),
        P(),
        P(),
    )
    return jax.shard_map(
        on_device, mesh=mesh, in_specs=placed, out_specs=P("head", "seq", None), check_vma=False
    )
```
